128 devices in a mesh: grp: 2 (over core), row: 8 (over z, y_hi), col: 8 (over y_lo, x).
Axes of the slice: x: 4, y: 4 (y_hi: 2, y_lo: 2; y = y_hi * 2 + y_lo), z: 4, core: 2. Of those that a mesh axis runs over, the one named last changes fastest.
Arguments:
- ainv_anc: bfloat16 [12288, 12288], P(('grp', 'row'), 'col'), may hold values from -12 to 12
- l_upper: bfloat16 [12288, 2048], P(('grp', 'row'), 'col'), may hold values from -0.0546875 to 0.0546875
- mask_upper: int32 [8, 48], replicated, may hold values from 0 to 1, as said below
- dinv_upper: float32 [256, 2048], P(None, 'col'), may hold values from -6 to 6
- l_lower: bfloat16 [12288, 2048], P(('grp', 'row'), 'col'), may hold values from -0.0546875 to 0.0546875
- mask_lower: int32 [8, 48], replicated, may hold values from 0 to 1, as said below
- parent: int32 [8], replicated, may hold values from 0 to 7
- lp_lower: bfloat16 [256, 2048], P(None, 'col'), may hold values from -0.375 to 0.375
- dinv_lower: float32 [256, 2048], P(None, 'col'), may hold values from -6 to 6
Outputs:
- x_upper: bfloat16 [12288, 2048], P(('grp', 'row'), 'col')
- diag_upper: bfloat16 [256, 2048], P(None, 'col')
- y_lower: bfloat16 [12288, 2048], P(('grp', 'row'), 'col')
- y_parent: bfloat16 [256, 2048], P(None, 'col')
- diag_lower: bfloat16 [256, 2048], P(None, 'col')
The draws below stay inside these ranges and needn't reach their ends.
Inputs may be any that keep to these rules, and one draw needn't show every extreme that they name: mask_upper[u, a] is 1 where ancestor block a lies in the structure of upper supernode u. mask_lower[l, a] is 1 where ancestor block a lies in the structure of lower supernode l. parent[l] is the upper supernode whose columns hold lower supernode l's parent block.
All inputs are finite; a program needn't handle non-finite values.
Results may differ from the reference program's by a relative error of at most 0.0095.
Values may be sent and summed in bfloat16 or wider, within the bound.
No kernel may reach another device: no remote copies, remote signals or barrier semaphores. Data moves between devices by JAX's collectives and lax.ppermute only.
A program may use at most 128 MiB of HBM per device.

```python
import jax
import jax.numpy as jnp
from jax import lax

B = 256
ANC = 12288
ANCB = 48
SN = 8


def draw_ainv_anc(key, part):
    entry_key, diag_key = jax.random.split(key, 2)
    entries = jnp.clip(jax.random.normal(entry_key, (ANC, ANC), jnp.float32), -7.0, 7.0)
    diagonal = jnp.exp(jax.random.uniform(diag_key, (ANC,), jnp.float32, 0.0, 1.386))
    places = jnp.arange(ANC)
    return entries.at[places, places].add(diagonal).astype(jnp.bfloat16)


def pattern_draw(key):
    chance = jax.random.randint(key, (SN, ANCB), 0, 1000)
    threshold = 250 + 650 * jnp.arange(ANCB, dtype=jnp.int32) // max(ANCB - 1, 1)
    return (chance < threshold[None, :]).astype(jnp.int32)


def draw_mask_upper(key, part):
    return pattern_draw(jax.random.fold_in(key, 17))


def draw_mask_lower(key, part):
    return pattern_draw(jax.random.fold_in(key, 29))


def plant(drawn, own_key, smallest, high):
    dims = drawn.shape
    place = [jax.random.randint(jax.random.fold_in(own_key, axis), (), 0, dims[axis]) for axis in range(len(dims))]
    drawn = drawn.at[tuple(place)].set(smallest)
    longest = dims.index(max(dims))
    place[longest] = (place[longest] + 1) % dims[longest]
    return drawn.at[tuple(place)].set(high)


def levels(stream_key, shape, cuts, smallest, high):
    def one(position, shards_of):
        heights = jax.random.uniform(jax.random.fold_in(jax.random.fold_in(stream_key, 6), position), (shards_of,), jnp.float32, smallest / len(cuts), high / len(cuts))
        return jnp.repeat(jnp.exp(heights), shape[position] // shards_of).reshape((-1,) + (1,) * (len(shape) - position - 1))

    gain = one(*cuts[0])
    for cut in cuts[1:]:
        gain = gain * one(*cut)
    return gain


def noise(rng, extent, width, bound, cuts=(), kind=jnp.bfloat16):
    values = jax.random.normal(rng, extent, jnp.float32) * width
    if len(cuts) > 0:
        values = levels(rng, extent, cuts, -0.22, 0.18) * values
    return jnp.clip(values, min=-bound, max=bound).astype(kind)


def setup_inputs(seed: int = 0) -> dict:
    keys = jax.random.split(jax.random.key(seed), 10)
    return {
        "ainv_anc": draw_ainv_anc(jax.random.fold_in(keys[9], 71), 0),
        "l_upper": noise(keys[1], (ANC, SN * B), ANC ** -0.5, 0.0546875, ((0, 16), (1, 8))),
        "mask_upper": draw_mask_upper(jax.random.fold_in(keys[9], 71), 0),
        "dinv_upper": noise(keys[3], (B, SN * B), 1.0, 6.0, ((1, 8),), jnp.float32),
        "l_lower": noise(keys[4], (ANC, SN * B), ANC ** -0.5, 0.0546875, ((0, 16), (1, 8))),
        "mask_lower": draw_mask_lower(jax.random.fold_in(keys[9], 71), 0),
        "parent": plant(jax.random.randint(keys[6], (SN,), 0, SN), jax.random.fold_in(keys[6], 1), 0, SN - 1).astype(jnp.int32),
        "lp_lower": noise(keys[7], (B, SN * B), B ** -0.5, 0.375, ((1, 8),)),
        "dinv_lower": noise(keys[8], (B, SN * B), 1.0, 6.0, ((1, 8),), jnp.float32),
    }


def masked_panel(factor, pattern):
    height, breadth = factor.shape
    shaped = factor.reshape(height // B, B, breadth // B, B)
    keeping = (jnp.transpose(pattern) > 0)[:, None, :, None]
    return jnp.where(keeping, shaped, jnp.zeros((), factor.dtype)).reshape(height, breadth)


def reference(ainv_anc, l_upper, mask_upper, dinv_upper, l_lower, mask_lower, parent, lp_lower, dinv_lower):
    precise = lax.Precision.HIGHEST
    ancestor = ainv_anc.astype(jnp.float32)
    upper_masked = masked_panel(l_upper, mask_upper)
    x_upper = (-jnp.dot(ancestor, upper_masked.astype(jnp.float32), precision=precise)).astype(jnp.bfloat16)
    upper_cube = upper_masked.astype(jnp.float32).reshape(ANC, SN, B)
    x_cube = x_upper.astype(jnp.float32).reshape(ANC, SN, B)
    upper_terms = jnp.einsum("aub,auc->buc", upper_cube, x_cube, precision=precise).reshape(B, SN * B)
    diag_upper = (dinv_upper - upper_terms).astype(jnp.bfloat16)
    lower_masked = masked_panel(l_lower, mask_lower)
    lower_cube = lower_masked.astype(jnp.float32).reshape(ANC, SN, B)
    chosen = jnp.take(x_cube, parent, axis=1)
    link_cube = lp_lower.astype(jnp.float32).reshape(B, SN, B)
    coupling = jnp.einsum("alb,blc->alc", chosen, link_cube, precision=precise).reshape(ANC, SN * B)
    lower_sum = jnp.dot(ancestor, lower_masked.astype(jnp.float32), precision=precise)
    y_lower = (-(lower_sum + coupling)).astype(jnp.bfloat16)
    y_cube = y_lower.astype(jnp.float32).reshape(ANC, SN, B)
    crossed = jnp.einsum("alb,alc->blc", chosen, lower_cube, precision=precise)
    own_terms = jnp.einsum("alb,alc->blc", lower_cube, y_cube, precision=precise)
    parent_diag = jnp.take(diag_upper.astype(jnp.float32).reshape(B, SN, B), parent, axis=1)
    parent_terms = jnp.einsum("blc,cld->bld", parent_diag, link_cube, precision=precise)
    y_parent = (-(crossed + parent_terms)).astype(jnp.bfloat16)
    parent_cube = y_parent.astype(jnp.float32)
    back_terms = jnp.einsum("clb,cld->bld", link_cube, parent_cube, precision=precise)
    diag_lower = (dinv_lower.reshape(B, SN, B) - own_terms - back_terms).astype(jnp.bfloat16)
    return x_upper, diag_upper, y_lower, y_parent.reshape(B, SN * B), diag_lower.reshape(B, SN * B)
```

```python
import functools

import jax
import jax.numpy as jnp
import numpy as np
from jax import lax
from jax.experimental import pallas as pl
from jax.experimental.pallas import tpu as pltpu
from jax.sharding import PartitionSpec as P

ALL = ("grp", "row", "col")
GR = ("grp", "row")
SHAPE = (2, 4, 2, 2, 4)
BF = jnp.bfloat16
F32 = jnp.float32


def perm(move):
    pairs = []
    for place in np.ndindex(*SHAPE):
        target = move(*place)
        pairs.append(
            (int(np.ravel_multi_index(place, SHAPE)), int(np.ravel_multi_index(target, SHAPE)))
        )
    return pairs


TURN = perm(lambda g, z, h, v, x: (v, x, h, g, z))
CORE = perm(lambda g, z, h, v, x: (1 - g, z, h, v, x))
Y_HI = perm(lambda g, z, h, v, x: (g, z, 1 - h, v, x))
Y_LO = perm(lambda g, z, h, v, x: (g, z, h, 1 - v, x))
Z_UP = perm(lambda g, z, h, v, x: (g, (z + 1) % 4, h, v, x))
Z_DOWN = perm(lambda g, z, h, v, x: (g, (z - 1) % 4, h, v, x))
X_UP = perm(lambda g, z, h, v, x: (g, z, h, v, (x + 1) % 4))
X_DOWN = perm(lambda g, z, h, v, x: (g, z, h, v, (x - 1) % 4))
LAST_A = perm(lambda g, z, h, v, x: (1 - g, z, h, v, x) if g == v else (g, z, h, 1 - v, x))
LAST_B = perm(lambda g, z, h, v, x: (g, z, h, v, x) if g == v else (1 - g, z, h, 1 - v, x))


def send(value, pairs, name):
    with jax.named_scope(name):
        return lax.ppermute(value, ALL, pairs)


def dot(a, b, contract):
    return lax.dot_general(a, b, ((contract[:1], contract[1:]), ((), ())), preferred_element_type=F32)


def products_kernel(coupled, depth, rows, scal, *refs):
    n_in = 10 + (3 if coupled else 0)
    a_ref, ap_ref = refs[0], refs[1]
    pieces = refs[2:10]
    outs = refs[n_in : n_in + 5]
    a_s, b_s, sems = refs[n_in + 5 :]
    half, offset = scal[0], scal[1]
    copies = []
    for block, source in enumerate((a_ref, ap_ref)):
        for part in range(2):
            which = half if part == 0 else 1 - half
            copies.append(
                pltpu.make_async_copy(
                    source.at[:, pl.ds(pl.multiple_of(which * depth, depth), depth)],
                    a_s.at[pl.ds(block * rows, rows), pl.ds(part * depth, depth)],
                    sems.at[len(copies)],
                )
            )
    for k in range(4):
        slot = lax.rem(k - offset + 4, 4)
        for part in range(2):
            copies.append(
                pltpu.make_async_copy(
                    pieces[part * 4 + k],
                    b_s.at[slot, pl.ds(part * depth, depth), :],
                    sems.at[len(copies)],
                )
            )
    for copy in copies:
        copy.start()
    for copy in copies:
        copy.wait()
    plus, minus, later_plus, later_minus, keep = outs
    own, across = pl.ds(0, rows), pl.ds(rows, rows)
    targets = {
        (2, 0): (plus, own),
        (1, 1): (plus, across),
        (3, 0): (minus, own),
        (2, 1): (minus, across),
        (1, 0): (later_plus, own),
        (3, 1): (later_minus, own),
        (0, 0): (keep, own),
        (0, 1): (keep, across),
    }
    for (j, block), (target, place) in targets.items():
        total = jnp.dot(
            a_s[pl.ds(block * rows, rows), :], b_s[j], preferred_element_type=F32
        )
        if coupled:
            total += jnp.dot(refs[10 + block][...], refs[12][j], preferred_element_type=F32)
        target[place, :] = total.astype(target.dtype)


def products(scal, a, a_across, pieces, coupling=()):
    rows, width = a.shape
    depth, b = pieces[0].shape
    coupled = len(coupling) > 0
    vmem = pl.BlockSpec(memory_space=pltpu.VMEM)
    hbm = pl.BlockSpec(memory_space=pl.ANY)
    shapes = [
        jax.ShapeDtypeStruct((2 * rows, b), BF),
        jax.ShapeDtypeStruct((2 * rows, b), BF),
        jax.ShapeDtypeStruct((rows, b), BF),
        jax.ShapeDtypeStruct((rows, b), BF),
        jax.ShapeDtypeStruct((2 * rows, b), BF),
    ]
    return pl.pallas_call(
        functools.partial(products_kernel, coupled, depth, rows),
        out_shape=shapes,
        in_specs=[pl.BlockSpec(memory_space=pltpu.SMEM)] + [hbm] * 10 + [vmem] * len(coupling),
        out_specs=[vmem] * 5,
        scratch_shapes=[
            pltpu.VMEM((2 * rows, width), BF),
            pltpu.VMEM((4, width, b), BF),
            pltpu.SemaphoreType.DMA((12,)),
        ],
        cost_estimate=pl.CostEstimate(
            flops=2 * 2 * rows * width * 4 * b, bytes_accessed=12_000_000, transcendentals=0
        ),
        compiler_params=pltpu.CompilerParams(vmem_limit_bytes=28 * 1024 * 1024),
        name="products",
    )(scal, a, a_across, *pieces, *coupling)


def plain_products(scal, a, a_across, pieces, coupling=()):
    rows, _ = a.shape
    depth, b = pieces[0].shape
    half, offset = scal[0], scal[1]
    full = jnp.concatenate([a, a_across], 0).astype(F32)
    full = jnp.where(half == 0, full, jnp.roll(full, depth, axis=1))
    stack = jnp.stack([jnp.concatenate([pieces[k], pieces[4 + k]], 0) for k in range(4)])
    c = [full @ jnp.take(stack, (offset + j) % 4, axis=0).astype(F32) for j in range(4)]
    if coupling:
        x2 = jnp.concatenate(coupling[:2], 0).astype(F32)
        c = [c[j] + x2 @ coupling[2][j].astype(F32) for j in range(4)]
    c = [v.astype(BF) for v in c]
    return (
        jnp.concatenate([c[2][:rows], c[1][rows:]]),
        jnp.concatenate([c[3][:rows], c[2][rows:]]),
        c[1][:rows],
        c[3][rows:],
        c[0],
    )


def solution(mesh, multiply=products):
    def body(a, l_up, m_up, d_up, l_lo, m_lo, parent, lp, d_lo):
        rows, b = l_up.shape
        blocks = rows // b
        piece = b // 16
        g, row, col = lax.axis_index("grp"), lax.axis_index("row"), lax.axis_index("col")
        z, h = row // 2, row % 2
        v, x = col // 4, col % 4
        place = g * 8 + row

        def masked(factor, pattern):
            keep = lax.dynamic_slice(pattern, (col, place * blocks), (1, blocks)) > 0
            shaped = factor.reshape(blocks, b, b)
            return jnp.where(keep.reshape(blocks, 1, 1), shaped, jnp.zeros((), BF)).reshape(rows, b)

        up, lo = masked(l_up, m_up), masked(l_lo, m_lo)
        a_across = send(a, CORE, "a_core")
        scal = jnp.stack([h, (x - z) % 4]).astype(jnp.int32)

        def spread(panel, name):
            k0 = send(panel, TURN, name + "_turn")
            o0 = send(k0, Y_HI, name + "_hi")
            k3 = send(k0, Z_UP, name + "_k3")
            k1 = send(k0, Z_DOWN, name + "_k1")
            o3 = send(o0, Z_UP, name + "_o3")
            o1 = send(o0, Z_DOWN, name + "_o1")
            k2 = send(k3, Z_UP, name + "_k2")
            o2 = send(o1, Z_DOWN, name + "_o2")
            return k0, k1, k2, k3, o0, o1, o2, o3

        def reduce(parts, name):
            plus, minus, later_plus, later_minus, keep = parts
            r1 = send(plus, X_UP, name + "_r1")
            r3 = send(minus, X_DOWN, name + "_r3")
            s1 = (later_plus.astype(F32) + r1[:rows].astype(F32)).astype(BF)
            s3 = (later_minus.astype(F32) + r3[rows:].astype(F32)).astype(BF)
            q1 = send(s1, X_UP, name + "_q1")
            q3 = send(s3, X_DOWN, name + "_q3")
            mine = keep[:rows].astype(F32) + r3[:rows].astype(F32) + q1.astype(F32)
            other = keep[rows:].astype(F32) + r1[rows:].astype(F32) + q3.astype(F32)
            same = g == v
            first = jnp.where(same, other, mine).astype(BF)
            second = jnp.where(same, mine, other).astype(BF)
            first = send(first, LAST_A, name + "_la")
            second = send(second, LAST_B, name + "_lb")
            return (-(first.astype(F32) + second.astype(F32))).astype(BF)

        up_pieces = spread(up, "u")
        lo_pieces = spread(lo, "l")

        both = jnp.concatenate([lo, lp], 0)
        both = jnp.concatenate([both, send(both, Y_LO, "c_lo")], 0)
        c3 = send(both, X_UP, "c_3")
        c1 = send(both, X_DOWN, "c_1")
        size = rows + b
        c2a = send(c3[:size], X_UP, "c_2a")
        c2b = send(c1[size:], X_DOWN, "c_2b")
        near = [both[:size], c1[:size], c2a, c3[:size]]
        far = [both[size:], c1[size:], c2b, c3[size:]]
        around = (x + jnp.arange(4)) % 4
        link_near = jnp.stack([n[rows:] for n in near])
        link_far = jnp.stack([n[rows:] for n in far])
        is_near = parent[4 * v + around] == col
        is_far = parent[4 * (1 - v) + around] == col

        x_own = reduce(multiply(scal, a, a_across, up_pieces), "x")
        x_across = send(x_own, CORE, "x_core")
        links = jnp.where(
            jnp.where(g == v, is_near, is_far)[:, None, None],
            jnp.where(g == v, link_near, link_far),
            jnp.zeros((), BF),
        )

        y_own = reduce(
            multiply(scal, a, a_across, lo_pieces, (x_own, x_across, links)), "y"
        )

        pieces = [dot(up, x_own, (0, 0))]
        for chosen, flags in ((near, is_near), (far, is_far)):
            for k in range(4):
                crossed = dot(x_own, chosen[k][:rows], (0, 0))
                pieces.append(jnp.where(flags[k], crossed, 0.0))
        wide = jnp.concatenate([p.astype(BF) for p in pieces], 1).reshape(16, piece, 9 * b)
        with jax.named_scope("sum_upper"):
            wide = lax.all_to_all(wide, GR, 0, 0, tiled=True)
        wide = jnp.sum(wide.astype(F32), 0)
        start = place * piece
        d_slice = (lax.dynamic_slice(d_up, (start, 0), (piece, b)) - wide[:, :b]).astype(BF)
        terms = []
        for n, (link, flags) in enumerate(((link_near, is_near), (link_far, is_far))):
            part = []
            for k in range(4):
                at = (1 + 4 * n + k) * b
                term = wide[:, at : at + b] + dot(d_slice, link[k], (1, 0))
                part.append(jnp.where(flags[k], term, 0.0).astype(BF))
            terms.append(jnp.roll(jnp.stack(part), x, axis=0))
        ordered = jnp.where(
            v == 0, jnp.concatenate(terms, 0), jnp.concatenate(terms[::-1], 0)
        )
        with jax.named_scope("to_child"):
            ordered = lax.all_to_all(ordered, "col", 0, 0, tiled=True)
        p_slice = (-jnp.sum(ordered.astype(F32), 0)).astype(BF)
        out = jnp.concatenate([d_slice, p_slice], 1)
        with jax.named_scope("share_upper"):
            out = lax.all_to_all(
                jnp.broadcast_to(out[None], (16, piece, 2 * b)), GR, 0, 0, tiled=True
            ).reshape(b, 2 * b)
        diag_up, y_parent = out[:, :b], out[:, b:]

        lp_slice = lax.dynamic_slice(lp, (start, 0), (piece, b))
        own = dot(lo, y_own, (0, 0)) + dot(lp_slice, p_slice, (0, 0))
        with jax.named_scope("sum_lower"):
            own = lax.all_to_all(own.astype(BF).reshape(16, piece, b), GR, 0, 0, tiled=True)
        own = jnp.sum(own.astype(F32), 0)
        last = (lax.dynamic_slice(d_lo, (start, 0), (piece, b)) - own).astype(BF)
        with jax.named_scope("share_lower"):
            last = lax.all_to_all(
                jnp.broadcast_to(last[None], (16, piece, b)), GR, 0, 0, tiled=True
            ).reshape(b, b)
        return x_own, diag_up, y_own, y_parent, last

    tall, flat, full = P(GR, "col"), P(None, "col"), P(None, None)
    return jax.shard_map(
        body,
        mesh=mesh,
        in_specs=(tall, tall, full, flat, tall, full, P(None), flat, flat),
        out_specs=(tall, flat, tall, flat, flat),
        check_vma=False,
    )
```

```python
import functools

import jax
import jax.numpy as jnp
import numpy as np
from jax import lax
from jax.experimental import pallas as pl
from jax.experimental.pallas import tpu as pltpu
from jax.sharding import PartitionSpec as P


ALL = ("grp", "row", "col")
GR = ("grp", "row")
SHAPE = (2, 4, 2, 2, 4)
BF = jnp.bfloat16
F32 = jnp.float32


def perm(move):
    pairs = []
    for place in np.ndindex(*SHAPE):
        target = move(*place)
        pairs.append(
            (int(np.ravel_multi_index(place, SHAPE)), int(np.ravel_multi_index(target, SHAPE)))
        )
    return pairs


TURN = perm(lambda g, z, h, v, x: (v, -x % 4, h, g, z))
CORE = perm(lambda g, z, h, v, x: (1 - g, z, h, v, x))
Y_HI = perm(lambda g, z, h, v, x: (g, z, 1 - h, v, x))
Y_LO = perm(lambda g, z, h, v, x: (g, z, h, 1 - v, x))
Z_UP = perm(lambda g, z, h, v, x: (g, (z + 1) % 4, h, v, x))
Z_DOWN = perm(lambda g, z, h, v, x: (g, (z - 1) % 4, h, v, x))
X_UP = perm(lambda g, z, h, v, x: (g, z, h, v, (x + 1) % 4))
X_DOWN = perm(lambda g, z, h, v, x: (g, z, h, v, (x - 1) % 4))
LAST_A = perm(lambda g, z, h, v, x: (1 - g, z, h, v, x) if g == v else (g, z, h, 1 - v, x))
LAST_B = perm(lambda g, z, h, v, x: (g, z, h, v, x) if g == v else (1 - g, z, h, 1 - v, x))


def send(value, pairs):
    return lax.ppermute(value, ALL, pairs)


def dot(a, b, contract):
    return lax.dot_general(a, b, ((contract[:1], contract[1:]), ((), ())), preferred_element_type=F32)


def targets_of(rows):
    own, across = pl.ds(0, rows), pl.ds(rows, rows)
    return (
        (2, 0, 0, own),
        (3, 0, 1, own),
        (1, 0, 2, own),
        (0, 0, 4, own),
        (1, 1, 0, across),
        (2, 1, 1, across),
        (3, 1, 3, own),
        (0, 1, 4, across),
    )


CHUNKS = 3


def products_kernel(depth, rows, scal, *refs):
    pieces = refs[2:10]
    outs = refs[10:15]
    a_s, b_s, c_s, a_sems, b_sems, c_sems = refs[15:]
    half, offset = scal[0], scal[1]
    size = rows // CHUNKS
    b = c_s.shape[2]

    def a_copy(chunk, part):
        which = half if part == 0 else 1 - half
        block, step = divmod(chunk, CHUNKS)
        return pltpu.make_async_copy(
            refs[block].at[
                pl.ds(step * size, size), pl.ds(pl.multiple_of(which * depth, depth), depth)
            ],
            a_s.at[pl.ds(chunk * size, size), pl.ds(part * depth, depth)],
            a_sems.at[chunk, part],
        )

    def b_copy(piece, slot, part):
        return pltpu.make_async_copy(
            pieces[piece],
            b_s.at[pl.ds(part * depth, depth), pl.ds(pl.multiple_of(slot * b, b), b)],
            b_sems.at[slot, part],
        )

    for part in range(2):
        a_copy(0, part).start()
        for k in range(4):
            b_copy(part * 4 + k, lax.rem(offset - k + 4, 4), part).start()
    for chunk in range(1, 2 * CHUNKS):
        a_copy(chunk, 0).start()
        a_copy(chunk, 1).start()
    for j in range(4):
        b_copy(0, j, 0).wait()
        b_copy(0, j, 1).wait()
    copies = []
    for chunk in range(2 * CHUNKS):
        a_copy(chunk, 0).wait()
        a_copy(chunk, 1).wait()
        block, step = divmod(chunk, CHUNKS)
        total = jnp.dot(
            a_s[pl.ds(chunk * size, size), :], b_s[...], preferred_element_type=F32
        ).astype(BF)
        for n, (j, where, out, place) in enumerate(targets_of(rows)):
            if where == block:
                c_s[n, pl.ds(step * size, size), :] = total[:, j * b : (j + 1) * b]
                copies.append(
                    pltpu.make_async_copy(
                        c_s.at[n, pl.ds(step * size, size), :],
                        outs[out].at[pl.ds(place.start + step * size, size), :],
                        c_sems.at[n, step],
                    )
                )
                copies[-1].start()
    for copy in copies:
        copy.wait()


def products(scal, a, a_across, pieces):
    rows, width = a.shape
    depth, b = pieces[0].shape
    tall, short = jax.ShapeDtypeStruct((2 * rows, b), BF), jax.ShapeDtypeStruct((rows, b), BF)
    hbm = pl.BlockSpec(memory_space=pl.ANY)
    return pl.pallas_call(
        functools.partial(products_kernel, depth, rows),
        out_shape=[tall, tall, short, short, tall],
        in_specs=[pl.BlockSpec(memory_space=pltpu.SMEM)] + [hbm] * 10,
        out_specs=[hbm] * 5,
        scratch_shapes=[
            pltpu.VMEM((2 * rows, width), BF),
            pltpu.VMEM((width, 4 * b), BF),
            pltpu.VMEM((8, rows, b), BF),
            pltpu.SemaphoreType.DMA((2 * CHUNKS, 2)),
            pltpu.SemaphoreType.DMA((4, 2)),
            pltpu.SemaphoreType.DMA((8, CHUNKS)),
        ],
        cost_estimate=pl.CostEstimate(
            flops=2 * 2 * rows * width * 4 * b, bytes_accessed=12_000_000, transcendentals=0
        ),
        compiler_params=pltpu.CompilerParams(vmem_limit_bytes=60 * 1024 * 1024),
        name="products",
    )(scal, a, a_across, *pieces)


NEAR = {0: 0, 1: 1, 3: 4}
FAR = {0: 5, 1: 6, 3: 9}


def link_at(j, far, rows, b):
    if j == 2:
        return 3, rows + far * b - (rows + 2 * b) // 2
    return NEAR[j], rows + far * b


def panel_at(j, far, rows, b):
    cut = rows // 2 if far else (rows + 2 * b) // 2
    if j != 2:
        return (((FAR if far else NEAR)[j], 0, 0, rows),)
    first, second = (7, 8) if far else (2, 3)
    return (first, 0, 0, cut), (second, 0, cut, rows - cut)


def couple_kernel(rows, scal, parent, x_own, x_across, *refs):
    cols, outs = refs[:5], refs[10:15]
    blocks, links, in_sems, out_sems, link_sems = refs[15:]
    col, v, x, g = scal[2], scal[3], scal[4], scal[5]
    b = links.shape[1]

    def used(j):
        return parent[4 * g + lax.rem(x + j, 4)] == col

    def block_in(n, out, place):
        return pltpu.make_async_copy(outs[out].at[place, :], blocks.at[n], in_sems.at[n])

    def block_out(n, out, place):
        return pltpu.make_async_copy(blocks.at[n], outs[out].at[place, :], out_sems.at[n])

    def link_in(j, far):
        buffer, at = link_at(j, far, rows, b)
        return pltpu.make_async_copy(
            cols[buffer].at[pl.ds(at, b), :], links.at[j], link_sems.at[j]
        )

    for j in range(4):
        for far in range(2):

            @pl.when(jnp.logical_and(used(j), (g == v) == (far == 0)))
            def _():
                link_in(j, far).start()

    for n, (j, block, out, place) in enumerate(targets_of(rows)):

        @pl.when(used(j))
        def _():
            block_in(n, out, place).start()

    for n, (j, block, out, place) in enumerate(targets_of(rows)):

        @pl.when(used(j))
        def _():
            if block == 0:
                link_in(j, 0).wait()
            block_in(n, out, place).wait()
            value = (x_own, x_across)[block]
            total = jnp.dot(value[...], links[j], preferred_element_type=F32)
            blocks[n] = (blocks[n].astype(F32) + total).astype(BF)
            block_out(n, out, place).start()

    for n, (j, block, out, place) in enumerate(targets_of(rows)):

        @pl.when(used(j))
        def _():
            block_out(n, out, place).wait()


def couple(scal, parent, parts, x_own, x_across, cols):
    rows, b = x_own.shape
    smem = pl.BlockSpec(memory_space=pltpu.SMEM)
    vmem = pl.BlockSpec(memory_space=pltpu.VMEM)
    hbm = pl.BlockSpec(memory_space=pl.ANY)
    return pl.pallas_call(
        functools.partial(couple_kernel, rows),
        out_shape=[jax.ShapeDtypeStruct(p.shape, BF) for p in parts],
        in_specs=[smem, smem, vmem, vmem] + [hbm] * 10,
        out_specs=[hbm] * 5,
        scratch_shapes=[
            pltpu.VMEM((8, rows, b), BF),
            pltpu.VMEM((4, b, b), BF),
            pltpu.SemaphoreType.DMA((8,)),
            pltpu.SemaphoreType.DMA((8,)),
            pltpu.SemaphoreType.DMA((4,)),
        ],
        input_output_aliases={9 + n: n for n in range(5)},
        cost_estimate=pl.CostEstimate(
            flops=2 * 2 * rows * b * 4 * b, bytes_accessed=8_000_000, transcendentals=0
        ),
        compiler_params=pltpu.CompilerParams(vmem_limit_bytes=60 * 1024 * 1024),
        name="couple",
    )(scal, parent, x_own, x_across, *cols, *parts)


def crossed_kernel(rows, scal, parent, x_ref, up_ref, d_ref, *refs):
    cols, (upper, terms, held, sems) = refs[:10], refs[10:]
    col, v, x, place = scal[2], scal[3], scal[4], scal[6]
    slices, _, piece, b = terms.shape

    def child(n):
        side = v if n < 4 else 1 - v
        return 4 * side + lax.rem(x + n % 4, 4)

    def fetch(n):
        far, j = divmod(n, 4)
        buffer, at = link_at(j, far, rows, b)
        parts = panel_at(j, far, rows, b) + ((buffer, at, rows, b),)
        return [
            pltpu.make_async_copy(
                cols[source].at[pl.ds(start, size), :],
                held.at[n, pl.ds(to, size), :],
                sems.at[n, m],
            )
            for m, (source, start, to, size) in enumerate(parts)
        ]

    for n in range(8):

        @pl.when(parent[child(n)] == col)
        def _():
            for copy in fetch(n):
                copy.start()

    total = dot(up_ref[...], x_ref[...], (0, 0))
    upper[...] = total
    first = jnp.where(place == 0, 1.0, 0.0)
    diag = (d_ref[...] * first - total).astype(BF)
    for n in range(8):
        l = child(n)

        @pl.when(parent[l] == col)
        def _():
            for copy in fetch(n):
                copy.wait()
            term = dot(x_ref[...], held[n, pl.ds(0, rows), :], (0, 0))
            term += dot(diag, held[n, pl.ds(rows, b), :], (1, 0))
            terms[:, l] = term.astype(BF).reshape(slices, piece, b)

        @pl.when(parent[l] != col)
        def _():
            terms[:, l] = jnp.zeros((slices, piece, b), BF)


def crossed(scal, parent, x, up, d_up, cols):
    rows, b = x.shape
    smem = pl.BlockSpec(memory_space=pltpu.SMEM)
    vmem = pl.BlockSpec(memory_space=pltpu.VMEM)
    hbm = pl.BlockSpec(memory_space=pl.ANY)
    return pl.pallas_call(
        functools.partial(crossed_kernel, rows),
        out_shape=[
            jax.ShapeDtypeStruct((b, b), F32),
            jax.ShapeDtypeStruct((16, 8, b // 16, b), BF),
        ],
        in_specs=[smem, smem, vmem, vmem, vmem] + [hbm] * 10,
        out_specs=[vmem] * 2,
        scratch_shapes=[
            pltpu.VMEM((8, rows + b, b), BF),
            pltpu.SemaphoreType.DMA((8, 3)),
        ],
        cost_estimate=pl.CostEstimate(
            flops=2 * rows * b * 8 * b, bytes_accessed=5_000_000, transcendentals=0
        ),
        compiler_params=pltpu.CompilerParams(vmem_limit_bytes=60 * 1024 * 1024),
        name="crossed",
    )(scal, parent, x, up, d_up, *cols)


def after(value, *others):
    return lax.optimization_barrier((value,) + others)[0]


def solution(mesh):
    def body(a, l_up, m_up, d_up, l_lo, m_lo, parent, lp, d_lo):
        rows, b = l_up.shape
        blocks = rows // b
        piece = b // 16
        g, row, col = lax.axis_index("grp"), lax.axis_index("row"), lax.axis_index("col")
        z, h = row // 2, row % 2
        v, x = col // 4, col % 4
        place = g * 8 + row

        def masked(factor, pattern):
            keep = lax.dynamic_slice(pattern, (col, place * blocks), (1, blocks)) > 0
            shaped = factor.reshape(blocks, b, b)
            return jnp.where(keep.reshape(blocks, 1, 1), shaped, jnp.zeros((), BF)).reshape(rows, b)

        up, lo = masked(l_up, m_up), masked(l_lo, m_lo)
        a_across = send(a, CORE)
        scal = jnp.stack([h, (-x - z) % 4, col, v, x, g, place]).astype(jnp.int32)

        def spread(k0):
            o0 = send(k0, Y_HI)
            k3 = send(k0, Z_UP)
            k1 = send(k0, Z_DOWN)
            o3 = send(o0, Z_UP)
            o1 = send(o0, Z_DOWN)
            k2 = send(k3, Z_UP)
            o2 = send(o1, Z_DOWN)
            return k0, k1, k2, k3, o0, o1, o2, o3

        def reduce(parts):
            plus, minus, later_plus, later_minus, keep = parts
            r1 = send(plus, X_UP)
            r3 = send(minus, X_DOWN)
            s1 = (later_plus.astype(F32) + r1[:rows].astype(F32)).astype(BF)
            s3 = (later_minus.astype(F32) + r3[rows:].astype(F32)).astype(BF)
            q1 = send(s1, X_UP)
            q3 = send(s3, X_DOWN)
            mine = keep[:rows].astype(F32) + r3[:rows].astype(F32) + q1.astype(F32)
            other = keep[rows:].astype(F32) + r1[rows:].astype(F32) + q3.astype(F32)
            same = g == v
            first = jnp.where(same, other, mine).astype(BF)
            second = jnp.where(same, mine, other).astype(BF)
            first = send(first, LAST_A)
            second = send(second, LAST_B)
            return (-(first.astype(F32) + second.astype(F32))).astype(BF)

        up_pieces = spread(send(up, TURN))
        lo_first = send(after(lo, up_pieces[5]), TURN)

        own_col = jnp.concatenate([lo, lp, send(lp, Y_LO)], 0)
        cut = (rows + 2 * b) // 2
        own_col = after(own_col, up_pieces[0])
        n3 = send(own_col, X_UP)
        n1 = send(own_col, X_DOWN)
        n2a = send(n3[:cut], X_UP)
        n2b = send(n1[cut:], X_DOWN)
        far = send(lo, Y_LO)
        f3 = send(far, X_UP)
        f1 = send(far, X_DOWN)
        f2a = send(f3[: rows // 2], X_UP)
        f2b = send(f1[rows // 2 :], X_DOWN)
        near_cols = (own_col, n1, n2a, n2b, n3)
        cols = near_cols + (far, f1, f2a, f2b, f3)

        parts = products(scal, a, a_across, up_pieces)
        lo_pieces = spread(after(lo_first, parts[0]))
        x_own = reduce(parts)
        lo_parts = products(scal, a, a_across, lo_pieces)
        x_across = send(x_own, CORE)

        parts = couple(scal, parent, lo_parts, x_own, x_across, near_cols)
        y_own = reduce(parts)

        def halved(value):
            size = b // 2
            given = lax.dynamic_slice(value, ((1 - g) * size, 0), (size, b)).astype(BF)
            kept = lax.dynamic_slice(value, (g * size, 0), (size, b))
            return kept + send(given, CORE).astype(F32)

        upper, terms = crossed(scal, parent, x_own, up, d_up, cols)
        half = b // 2
        diag = halved(upper).astype(BF)
        diag = lax.all_to_all(jnp.broadcast_to(diag[None], (8, half, b)), "row", 0, 0, tiled=True)
        d_half = lax.dynamic_slice(d_up, (g * half, 0), (half, b)) - jnp.sum(diag.astype(F32), 0)

        terms = lax.all_to_all(after(terms, diag).reshape(128, piece, b), ALL, 0, 0, tiled=True)
        p_slice = (-jnp.sum(terms.astype(F32), 0)).astype(BF)

        own = halved(dot(lo, y_own, (0, 0))).astype(BF)
        own = jnp.concatenate([own, p_slice], 0)
        own = lax.all_to_all(jnp.broadcast_to(own[None], (8,) + own.shape), "row", 0, 0, tiled=True)
        last = lax.dynamic_slice(d_lo, (g * half, 0), (half, b)) - jnp.sum(
            own[:, :half].astype(F32), 0
        )
        y_parent = own[:, half:].reshape(half, b).astype(F32)
        mine = jnp.concatenate([d_half, y_parent, last], 1)
        other = send(mine, CORE)
        out = jnp.where(
            g == 0, jnp.concatenate([mine, other], 0), jnp.concatenate([other, mine], 0)
        )
        y_parent = out[:, b : 2 * b].astype(BF)
        last = out[:, 2 * b :] - dot(lp, y_parent, (0, 0))
        return x_own, out[:, :b].astype(BF), y_own, y_parent, last.astype(BF)

    tall, flat, full = P(GR, "col"), P(None, "col"), P(None, None)
    return jax.shard_map(
        body,
        mesh=mesh,
        in_specs=(tall, tall, full, flat, tall, full, P(None), flat, flat),
        out_specs=(tall, flat, tall, flat, flat),
        check_vma=False,
    )
```

```python
import functools

import jax
import jax.numpy as jnp
import numpy as np
from jax import lax
from jax.experimental import pallas as pl
from jax.experimental.pallas import tpu as pltpu
from jax.sharding import PartitionSpec as P


ALL = ("grp", "row", "col")
GR = ("grp", "row")
SHAPE = (2, 4, 2, 2, 4)
BF = jnp.bfloat16
F32 = jnp.float32


def perm(move):
    pairs = []
    for place in np.ndindex(*SHAPE):
        target = move(*place)
        pairs.append(
            (int(np.ravel_multi_index(place, SHAPE)), int(np.ravel_multi_index(target, SHAPE)))
        )
    return pairs


TURN = perm(lambda g, z, h, v, x: (v, -x % 4, h, g, z))
CORE = perm(lambda g, z, h, v, x: (1 - g, z, h, v, x))
Y_HI = perm(lambda g, z, h, v, x: (g, z, 1 - h, v, x))
Y_LO = perm(lambda g, z, h, v, x: (g, z, h, 1 - v, x))
Z_UP = perm(lambda g, z, h, v, x: (g, (z + 1) % 4, h, v, x))
Z_DOWN = perm(lambda g, z, h, v, x: (g, (z - 1) % 4, h, v, x))
X_FAR = perm(lambda g, z, h, v, x: (g, z, h, v, (x + 2) % 4))
Z_FAR = perm(lambda g, z, h, v, x: (g, (z + 2) % 4, h, v, x))
X_UP = perm(lambda g, z, h, v, x: (g, z, h, v, (x + 1) % 4))
X_DOWN = perm(lambda g, z, h, v, x: (g, z, h, v, (x - 1) % 4))
LAST_A = perm(lambda g, z, h, v, x: (1 - g, z, h, v, x) if g == v else (g, z, h, 1 - v, x))
LAST_B = perm(lambda g, z, h, v, x: (g, z, h, v, x) if g == v else (1 - g, z, h, 1 - v, x))


def send(value, pairs):
    return lax.ppermute(value, ALL, pairs)


def dot(a, b, contract):
    return lax.dot_general(a, b, ((contract[:1], contract[1:]), ((), ())), preferred_element_type=F32)


def targets_of(rows):
    own, across = pl.ds(0, rows), pl.ds(rows, rows)
    return (
        (2, 0, 0, own),
        (3, 0, 1, own),
        (1, 0, 2, own),
        (0, 0, 4, own),
        (1, 1, 0, across),
        (2, 1, 1, across),
        (3, 1, 3, own),
        (0, 1, 4, across),
    )


CHUNKS = 3


def products_kernel(depth, rows, scal, *refs):
    pieces = refs[2:10]
    outs = refs[10:15]
    a_s, b_s, c_s, a_sems, b_sems, c_sems = refs[15:]
    half, offset = scal[0], scal[1]
    size = rows // CHUNKS
    b = c_s.shape[2]

    def a_copy(chunk, part):
        which = half if part == 0 else 1 - half
        block, step = divmod(chunk, CHUNKS)
        return pltpu.make_async_copy(
            refs[block].at[
                pl.ds(step * size, size), pl.ds(pl.multiple_of(which * depth, depth), depth)
            ],
            a_s.at[pl.ds(chunk * size, size), pl.ds(part * depth, depth)],
            a_sems.at[chunk, part],
        )

    def b_copy(piece, slot, part):
        return pltpu.make_async_copy(
            pieces[piece],
            b_s.at[pl.ds(part * depth, depth), pl.ds(pl.multiple_of(slot * b, b), b)],
            b_sems.at[slot, part],
        )

    for part in range(2):
        a_copy(0, part).start()
        for k in range(4):
            b_copy(part * 4 + k, lax.rem(offset - k + 4, 4), part).start()
    for chunk in range(1, 2 * CHUNKS):
        a_copy(chunk, 0).start()
        a_copy(chunk, 1).start()
    for j in range(4):
        b_copy(0, j, 0).wait()
        b_copy(0, j, 1).wait()
    copies = []
    for chunk in range(2 * CHUNKS):
        a_copy(chunk, 0).wait()
        a_copy(chunk, 1).wait()
        block, step = divmod(chunk, CHUNKS)
        total = jnp.dot(
            a_s[pl.ds(chunk * size, size), :], b_s[...], preferred_element_type=F32
        ).astype(BF)
        for n, (j, where, out, place) in enumerate(targets_of(rows)):
            if where == block:
                c_s[n, pl.ds(step * size, size), :] = total[:, j * b : (j + 1) * b]
                copies.append(
                    pltpu.make_async_copy(
                        c_s.at[n, pl.ds(step * size, size), :],
                        outs[out].at[pl.ds(place.start + step * size, size), :],
                        c_sems.at[n, step],
                    )
                )
                copies[-1].start()
    for copy in copies:
        copy.wait()


def products(scal, a, a_across, pieces):
    rows, width = a.shape
    depth, b = pieces[0].shape
    tall, short = jax.ShapeDtypeStruct((2 * rows, b), BF), jax.ShapeDtypeStruct((rows, b), BF)
    hbm = pl.BlockSpec(memory_space=pl.ANY)
    return pl.pallas_call(
        functools.partial(products_kernel, depth, rows),
        out_shape=[tall, tall, short, short, tall],
        in_specs=[pl.BlockSpec(memory_space=pltpu.SMEM)] + [hbm] * 10,
        out_specs=[hbm] * 5,
        scratch_shapes=[
            pltpu.VMEM((2 * rows, width), BF),
            pltpu.VMEM((width, 4 * b), BF),
            pltpu.VMEM((8, rows, b), BF),
            pltpu.SemaphoreType.DMA((2 * CHUNKS, 2)),
            pltpu.SemaphoreType.DMA((4, 2)),
            pltpu.SemaphoreType.DMA((8, CHUNKS)),
        ],
        cost_estimate=pl.CostEstimate(
            flops=2 * 2 * rows * width * 4 * b, bytes_accessed=12_000_000, transcendentals=0
        ),
        compiler_params=pltpu.CompilerParams(vmem_limit_bytes=60 * 1024 * 1024),
        name="products",
    )(scal, a, a_across, *pieces)


def panel_at(n, rows):
    return n, 0, 0, rows


def link_at(n, rows, b):
    return n % 4, rows + n // 4 * b, rows, b


def couple_kernel(rows, scal, parent, x_own, x_across, *refs):
    cols, outs = refs[:4], refs[9:14]
    blocks, links, in_sems, out_sems, link_sems = refs[14:]
    col, v, x, g = scal[2], scal[3], scal[4], scal[5]
    b = links.shape[1]

    def used(j):
        return parent[4 * g + lax.rem(x + j, 4)] == col

    def block_in(n, out, place):
        return pltpu.make_async_copy(outs[out].at[place, :], blocks.at[n], in_sems.at[n])

    def block_out(n, out, place):
        return pltpu.make_async_copy(blocks.at[n], outs[out].at[place, :], out_sems.at[n])

    def link_in(j, far):
        buffer, start, _, size = link_at(j + 4 * far, rows, b)
        return pltpu.make_async_copy(
            cols[buffer].at[pl.ds(start, size), :], links.at[j], link_sems.at[j]
        )

    for j in range(4):
        for far in range(2):

            @pl.when(jnp.logical_and(used(j), (g == v) == (far == 0)))
            def _():
                link_in(j, far).start()

    for n, (j, block, out, place) in enumerate(targets_of(rows)):

        @pl.when(used(j))
        def _():
            block_in(n, out, place).start()

    for n, (j, block, out, place) in enumerate(targets_of(rows)):

        @pl.when(used(j))
        def _():
            if block == 0:
                link_in(j, 0).wait()
            block_in(n, out, place).wait()
            value = (x_own, x_across)[block]
            total = jnp.dot(value[...], links[j], preferred_element_type=F32)
            blocks[n] = (blocks[n].astype(F32) + total).astype(BF)
            block_out(n, out, place).start()

    for n, (j, block, out, place) in enumerate(targets_of(rows)):

        @pl.when(used(j))
        def _():
            block_out(n, out, place).wait()


def couple(scal, parent, parts, x_own, x_across, cols):
    rows, b = x_own.shape
    smem = pl.BlockSpec(memory_space=pltpu.SMEM)
    vmem = pl.BlockSpec(memory_space=pltpu.VMEM)
    hbm = pl.BlockSpec(memory_space=pl.ANY)
    return pl.pallas_call(
        functools.partial(couple_kernel, rows),
        out_shape=[jax.ShapeDtypeStruct(p.shape, BF) for p in parts],
        in_specs=[smem, smem, vmem, vmem] + [hbm] * 9,
        out_specs=[hbm] * 5,
        scratch_shapes=[
            pltpu.VMEM((8, rows, b), BF),
            pltpu.VMEM((4, b, b), BF),
            pltpu.SemaphoreType.DMA((8,)),
            pltpu.SemaphoreType.DMA((8,)),
            pltpu.SemaphoreType.DMA((4,)),
        ],
        input_output_aliases={8 + n: n for n in range(5)},
        cost_estimate=pl.CostEstimate(
            flops=2 * 2 * rows * b * 4 * b, bytes_accessed=8_000_000, transcendentals=0
        ),
        compiler_params=pltpu.CompilerParams(vmem_limit_bytes=60 * 1024 * 1024),
        name="couple",
    )(scal, parent, x_own, x_across, *cols, *parts)


def crossed_kernel(rows, scal, parent, x_ref, up_ref, d_ref, *refs):
    cols, (upper, terms, held, sems) = refs[:8], refs[8:]
    col, v, x, place = scal[2], scal[3], scal[4], scal[6]
    slices, _, piece, b = terms.shape

    def child(n):
        side = v if n < 4 else 1 - v
        return 4 * side + lax.rem(x + n % 4, 4)

    def fetch(n):
        parts = (panel_at(n, rows), link_at(n, rows, b))
        return [
            pltpu.make_async_copy(
                cols[source].at[pl.ds(start, size), :],
                held.at[n, pl.ds(to, size), :],
                sems.at[n, m],
            )
            for m, (source, start, to, size) in enumerate(parts)
        ]

    for n in range(8):

        @pl.when(parent[child(n)] == col)
        def _():
            for copy in fetch(n):
                copy.start()

    total = dot(up_ref[...], x_ref[...], (0, 0))
    upper[...] = total
    first = jnp.where(place == 0, 1.0, 0.0)
    diag = (d_ref[...] * first - total).astype(BF)
    for n in range(8):
        l = child(n)

        @pl.when(parent[l] == col)
        def _():
            for copy in fetch(n):
                copy.wait()
            term = dot(x_ref[...], held[n, pl.ds(0, rows), :], (0, 0))
            term += dot(diag, held[n, pl.ds(rows, b), :], (1, 0))
            terms[:, l] = term.astype(BF).reshape(slices, piece, b)

        @pl.when(parent[l] != col)
        def _():
            terms[:, l] = jnp.zeros((slices, piece, b), BF)


def crossed(scal, parent, x, up, d_up, cols):
    rows, b = x.shape
    smem = pl.BlockSpec(memory_space=pltpu.SMEM)
    vmem = pl.BlockSpec(memory_space=pltpu.VMEM)
    hbm = pl.BlockSpec(memory_space=pl.ANY)
    return pl.pallas_call(
        functools.partial(crossed_kernel, rows),
        out_shape=[
            jax.ShapeDtypeStruct((b, b), F32),
            jax.ShapeDtypeStruct((16, 8, b // 16, b), BF),
        ],
        in_specs=[smem, smem, vmem, vmem, vmem] + [hbm] * 8,
        out_specs=[vmem] * 2,
        scratch_shapes=[
            pltpu.VMEM((8, rows + b, b), BF),
            pltpu.SemaphoreType.DMA((8, 2)),
        ],
        cost_estimate=pl.CostEstimate(
            flops=2 * rows * b * 8 * b, bytes_accessed=5_000_000, transcendentals=0
        ),
        compiler_params=pltpu.CompilerParams(vmem_limit_bytes=60 * 1024 * 1024),
        name="crossed",
    )(scal, parent, x, up, d_up, *cols)


def after(value, *others):
    return lax.optimization_barrier((value,) + others)[0]


def solution(mesh):
    def body(a, l_up, m_up, d_up, l_lo, m_lo, parent, lp, d_lo):
        rows, b = l_up.shape
        blocks = rows // b
        piece = b // 16
        g, row, col = lax.axis_index("grp"), lax.axis_index("row"), lax.axis_index("col")
        z, h = row // 2, row % 2
        v, x = col // 4, col % 4
        place = g * 8 + row

        def masked(factor, pattern):
            keep = lax.dynamic_slice(pattern, (col, place * blocks), (1, blocks)) > 0
            shaped = factor.reshape(blocks, b, b)
            return jnp.where(keep.reshape(blocks, 1, 1), shaped, jnp.zeros((), BF)).reshape(rows, b)

        up, lo = masked(l_up, m_up), masked(l_lo, m_lo)
        a_across = send(a, CORE)
        scal = jnp.stack([h, (-x - z) % 4, col, v, x, g, place]).astype(jnp.int32)

        def spread(k0, direct):
            o0 = send(k0, Y_HI)
            k3 = send(k0, Z_UP)
            k1 = send(k0, Z_DOWN)
            o3 = send(o0, Z_UP)
            o1 = send(o0, Z_DOWN)
            k2 = send(k0, Z_FAR) if direct else send(k3, Z_UP)
            o2 = send(o0, Z_FAR) if direct else send(o1, Z_DOWN)
            return k0, k1, k2, k3, o0, o1, o2, o3

        def reduce(parts):
            plus, minus, later_plus, later_minus, keep = parts
            r1 = send(plus, X_UP)
            r3 = send(minus, X_DOWN)
            s1 = (later_plus.astype(F32) + r1[:rows].astype(F32)).astype(BF)
            s3 = (later_minus.astype(F32) + r3[rows:].astype(F32)).astype(BF)
            q1 = send(s1, X_UP)
            q3 = send(s3, X_DOWN)
            mine = keep[:rows].astype(F32) + r3[:rows].astype(F32) + q1.astype(F32)
            other = keep[rows:].astype(F32) + r1[rows:].astype(F32) + q3.astype(F32)
            same = g == v
            first = jnp.where(same, other, mine).astype(BF)
            second = jnp.where(same, mine, other).astype(BF)
            first = send(first, LAST_A)
            second = send(second, LAST_B)
            return (-(first.astype(F32) + second.astype(F32))).astype(BF)

        up_pieces = spread(send(up, TURN), False)
        lo_first = send(after(lo, up_pieces[2], up_pieces[6]), TURN)

        own_col = jnp.concatenate([lo, lp, send(lp, Y_LO)], 0)
        own_col = after(own_col, up_pieces[0])
        far = send(lo, Y_LO)
        n1, f1 = send(own_col, X_DOWN), send(far, X_DOWN)
        n2, f2 = send(own_col, X_FAR), send(far, X_FAR)
        n3, f3 = send(own_col, X_UP), send(far, X_UP)
        near_cols = (own_col, n1, n2, n3)
        cols = near_cols + (far, f1, f2, f3)

        parts = products(scal, a, a_across, up_pieces)
        lo_pieces = spread(after(lo_first, parts[0]), True)
        x_own = reduce(parts)
        lo_parts = products(scal, a, a_across, lo_pieces)
        x_across = send(x_own, CORE)

        parts = couple(scal, parent, lo_parts, x_own, x_across, near_cols)
        y_own = reduce(parts)

        def halved(value):
            size = b // 2
            given = lax.dynamic_slice(value, ((1 - g) * size, 0), (size, b)).astype(BF)
            kept = lax.dynamic_slice(value, (g * size, 0), (size, b))
            return kept + send(given, CORE).astype(F32)

        upper, terms = crossed(scal, parent, x_own, up, d_up, cols)
        terms = lax.all_to_all(terms.reshape(128, piece, b), ALL, 0, 0, tiled=True)
        p_slice = (-jnp.sum(terms.astype(F32), 0)).astype(BF)

        half = b // 2
        diag = halved(upper).astype(BF)
        diag = lax.all_to_all(jnp.broadcast_to(after(diag, p_slice)[None], (8, half, b)), "row", 0, 0, tiled=True)
        d_half = lax.dynamic_slice(d_up, (g * half, 0), (half, b)) - jnp.sum(diag.astype(F32), 0)

        own = halved(dot(lo, y_own, (0, 0))).astype(BF)
        own = jnp.concatenate([own, p_slice], 0)
        own = lax.all_to_all(jnp.broadcast_to(own[None], (8,) + own.shape), "row", 0, 0, tiled=True)
        last = lax.dynamic_slice(d_lo, (g * half, 0), (half, b)) - jnp.sum(
            own[:, :half].astype(F32), 0
        )
        y_parent = own[:, half:].reshape(half, b).astype(F32)
        mine = jnp.concatenate([d_half, y_parent, last], 1)
        other = send(mine, CORE)
        out = jnp.where(
            g == 0, jnp.concatenate([mine, other], 0), jnp.concatenate([other, mine], 0)
        )
        y_parent = out[:, b : 2 * b].astype(BF)
        last = out[:, 2 * b :] - dot(lp, y_parent, (0, 0))
        return x_own, out[:, :b].astype(BF), y_own, y_parent, last.astype(BF)

    tall, flat, full = P(GR, "col"), P(None, "col"), P(None, None)
    return jax.shard_map(
        body,
        mesh=mesh,
        in_specs=(tall, tall, full, flat, tall, full, P(None), flat, flat),
        out_specs=(tall, flat, tall, flat, flat),
        check_vma=False,
    )
```

```python
import functools

import jax
import jax.numpy as jnp
import numpy as np
from jax import lax
from jax.experimental import pallas as pl
from jax.experimental.pallas import tpu as pltpu
from jax.sharding import PartitionSpec as P


ALL = ("grp", "row", "col")
GR = ("grp", "row")
SHAPE = (2, 4, 2, 2, 4)
BF = jnp.bfloat16
F32 = jnp.float32


def perm(move):
    pairs = []
    for place in np.ndindex(*SHAPE):
        target = move(*place)
        pairs.append(
            (int(np.ravel_multi_index(place, SHAPE)), int(np.ravel_multi_index(target, SHAPE)))
        )
    return pairs


TURN = perm(lambda g, z, h, v, x: (v, -x % 4, h, g, z))
CORE = perm(lambda g, z, h, v, x: (1 - g, z, h, v, x))
Y_HI = perm(lambda g, z, h, v, x: (g, z, 1 - h, v, x))
Y_LO = perm(lambda g, z, h, v, x: (g, z, h, 1 - v, x))
Z_UP = perm(lambda g, z, h, v, x: (g, (z + 1) % 4, h, v, x))
Z_DOWN = perm(lambda g, z, h, v, x: (g, (z - 1) % 4, h, v, x))
X_FAR = perm(lambda g, z, h, v, x: (g, z, h, v, (x + 2) % 4))
Z_FAR = perm(lambda g, z, h, v, x: (g, (z + 2) % 4, h, v, x))
X_UP = perm(lambda g, z, h, v, x: (g, z, h, v, (x + 1) % 4))
X_DOWN = perm(lambda g, z, h, v, x: (g, z, h, v, (x - 1) % 4))
LAST_A = perm(lambda g, z, h, v, x: (1 - g, z, h, v, x) if g == v else (g, z, h, 1 - v, x))
LAST_B = perm(lambda g, z, h, v, x: (g, z, h, v, x) if g == v else (1 - g, z, h, 1 - v, x))


def send(value, pairs):
    return lax.ppermute(value, ALL, pairs)


def dot(a, b, contract):
    return lax.dot_general(a, b, ((contract[:1], contract[1:]), ((), ())), preferred_element_type=F32)


def targets_of(rows):
    own, across = pl.ds(0, rows), pl.ds(rows, rows)
    return (
        (2, 0, 0, own),
        (3, 0, 1, own),
        (1, 0, 2, own),
        (0, 0, 4, own),
        (1, 1, 0, across),
        (2, 1, 1, across),
        (3, 1, 3, own),
        (0, 1, 4, across),
    )


CHUNKS = 3


def products_kernel(depth, rows, scal, *refs):
    pieces = refs[2:10]
    outs = refs[10:15]
    a_s, b_s, c_s, a_sems, b_sems, c_sems = refs[15:]
    half, offset = scal[0], scal[1]
    size = rows // CHUNKS
    b = c_s.shape[2]

    def a_copy(chunk, part):
        which = half if part == 0 else 1 - half
        block, step = divmod(chunk, CHUNKS)
        return pltpu.make_async_copy(
            refs[block].at[
                pl.ds(step * size, size), pl.ds(pl.multiple_of(which * depth, depth), depth)
            ],
            a_s.at[pl.ds(chunk * size, size), pl.ds(part * depth, depth)],
            a_sems.at[chunk, part],
        )

    def b_copy(piece, slot, part):
        return pltpu.make_async_copy(
            pieces[piece],
            b_s.at[pl.ds(part * depth, depth), pl.ds(pl.multiple_of(slot * b, b), b)],
            b_sems.at[slot, part],
        )

    for part in range(2):
        a_copy(0, part).start()
        for k in range(4):
            b_copy(part * 4 + k, lax.rem(offset - k + 4, 4), part).start()
    for j in range(4):
        b_copy(0, j, 0).wait()
        b_copy(0, j, 1).wait()
    for chunk in range(1, 3):
        a_copy(chunk, 0).start()
        a_copy(chunk, 1).start()
    copies = []
    for chunk in range(2 * CHUNKS):
        a_copy(chunk, 0).wait()
        a_copy(chunk, 1).wait()
        if chunk + 3 < 2 * CHUNKS:
            a_copy(chunk + 3, 0).start()
            a_copy(chunk + 3, 1).start()
        block, step = divmod(chunk, CHUNKS)
        total = jnp.dot(
            a_s[pl.ds(chunk * size, size), :], b_s[...], preferred_element_type=F32
        ).astype(BF)
        for n, (j, where, out, place) in enumerate(targets_of(rows)):
            if where == block:
                c_s[n, pl.ds(step * size, size), :] = total[:, j * b : (j + 1) * b]
                copies.append(
                    pltpu.make_async_copy(
                        c_s.at[n, pl.ds(step * size, size), :],
                        outs[out].at[pl.ds(place.start + step * size, size), :],
                        c_sems.at[n, step],
                    )
                )
                copies[-1].start()
    for copy in copies:
        copy.wait()


def products(scal, a, a_across, pieces):
    rows, width = a.shape
    depth, b = pieces[0].shape
    tall, short = jax.ShapeDtypeStruct((2 * rows, b), BF), jax.ShapeDtypeStruct((rows, b), BF)
    hbm = pl.BlockSpec(memory_space=pl.ANY)
    return pl.pallas_call(
        functools.partial(products_kernel, depth, rows),
        out_shape=[tall, tall, short, short, tall],
        in_specs=[pl.BlockSpec(memory_space=pltpu.SMEM)] + [hbm] * 10,
        out_specs=[hbm] * 5,
        scratch_shapes=[
            pltpu.VMEM((2 * rows, width), BF),
            pltpu.VMEM((width, 4 * b), BF),
            pltpu.VMEM((8, rows, b), BF),
            pltpu.SemaphoreType.DMA((2 * CHUNKS, 2)),
            pltpu.SemaphoreType.DMA((4, 2)),
            pltpu.SemaphoreType.DMA((8, CHUNKS)),
        ],
        cost_estimate=pl.CostEstimate(
            flops=2 * 2 * rows * width * 4 * b, bytes_accessed=12_000_000, transcendentals=0
        ),
        compiler_params=pltpu.CompilerParams(vmem_limit_bytes=60 * 1024 * 1024),
        name="products",
    )(scal, a, a_across, *pieces)


def panel_at(n, rows):
    return n, 0, 0, rows


def link_at(n, rows, b):
    return n % 4, rows + n // 4 * b, rows, b


def couple_kernel(rows, scal, parent, x_own, x_across, *refs):
    cols, outs = refs[:4], refs[9:14]
    blocks, links, in_sems, out_sems, link_sems = refs[14:]
    col, v, x, g = scal[2], scal[3], scal[4], scal[5]
    b = links.shape[1]

    def used(j):
        return parent[4 * g + lax.rem(x + j, 4)] == col

    def block_in(n, out, place):
        return pltpu.make_async_copy(outs[out].at[place, :], blocks.at[n], in_sems.at[n])

    def block_out(n, out, place):
        return pltpu.make_async_copy(blocks.at[n], outs[out].at[place, :], out_sems.at[n])

    def link_in(j, far):
        buffer, start, _, size = link_at(j + 4 * far, rows, b)
        return pltpu.make_async_copy(
            cols[buffer].at[pl.ds(start, size), :], links.at[j], link_sems.at[j]
        )

    for j in range(4):
        for far in range(2):

            @pl.when(jnp.logical_and(used(j), (g == v) == (far == 0)))
            def _():
                link_in(j, far).start()

    for n, (j, block, out, place) in enumerate(targets_of(rows)):

        @pl.when(used(j))
        def _():
            block_in(n, out, place).start()

    for n, (j, block, out, place) in enumerate(targets_of(rows)):

        @pl.when(used(j))
        def _():
            if block == 0:
                link_in(j, 0).wait()
            block_in(n, out, place).wait()
            value = (x_own, x_across)[block]
            total = jnp.dot(value[...], links[j], preferred_element_type=F32)
            blocks[n] = (blocks[n].astype(F32) + total).astype(BF)
            block_out(n, out, place).start()

    for n, (j, block, out, place) in enumerate(targets_of(rows)):

        @pl.when(used(j))
        def _():
            block_out(n, out, place).wait()


def couple(scal, parent, parts, x_own, x_across, cols):
    rows, b = x_own.shape
    smem = pl.BlockSpec(memory_space=pltpu.SMEM)
    vmem = pl.BlockSpec(memory_space=pltpu.VMEM)
    hbm = pl.BlockSpec(memory_space=pl.ANY)
    return pl.pallas_call(
        functools.partial(couple_kernel, rows),
        out_shape=[jax.ShapeDtypeStruct(p.shape, BF) for p in parts],
        in_specs=[smem, smem, vmem, vmem] + [hbm] * 9,
        out_specs=[hbm] * 5,
        scratch_shapes=[
            pltpu.VMEM((8, rows, b), BF),
            pltpu.VMEM((4, b, b), BF),
            pltpu.SemaphoreType.DMA((8,)),
            pltpu.SemaphoreType.DMA((8,)),
            pltpu.SemaphoreType.DMA((4,)),
        ],
        input_output_aliases={8 + n: n for n in range(5)},
        cost_estimate=pl.CostEstimate(
            flops=2 * 2 * rows * b * 4 * b, bytes_accessed=8_000_000, transcendentals=0
        ),
        compiler_params=pltpu.CompilerParams(vmem_limit_bytes=60 * 1024 * 1024),
        name="couple",
    )(scal, parent, x_own, x_across, *cols, *parts)


def crossed_kernel(rows, scal, parent, x_ref, up_ref, d_ref, *refs):
    cols, (upper, terms, held, sems) = refs[:8], refs[8:]
    col, v, x, place = scal[2], scal[3], scal[4], scal[6]
    slices, _, piece, b = terms.shape

    def child(n):
        side = v if n < 4 else 1 - v
        return 4 * side + lax.rem(x + n % 4, 4)

    def fetch(n):
        parts = (panel_at(n, rows), link_at(n, rows, b))
        return [
            pltpu.make_async_copy(
                cols[source].at[pl.ds(start, size), :],
                held.at[n, pl.ds(to, size), :],
                sems.at[n, m],
            )
            for m, (source, start, to, size) in enumerate(parts)
        ]

    for n in range(8):

        @pl.when(parent[child(n)] == col)
        def _():
            for copy in fetch(n):
                copy.start()

    total = dot(up_ref[...], x_ref[...], (0, 0))
    upper[...] = total
    first = jnp.where(place == 0, 1.0, 0.0)
    diag = (d_ref[...] * first - total).astype(BF)
    for n in range(8):
        l = child(n)

        @pl.when(parent[l] == col)
        def _():
            for copy in fetch(n):
                copy.wait()
            term = dot(x_ref[...], held[n, pl.ds(0, rows), :], (0, 0))
            term += dot(diag, held[n, pl.ds(rows, b), :], (1, 0))
            terms[:, l] = term.astype(BF).reshape(slices, piece, b)

        @pl.when(parent[l] != col)
        def _():
            terms[:, l] = jnp.zeros((slices, piece, b), BF)


def crossed(scal, parent, x, up, d_up, cols):
    rows, b = x.shape
    smem = pl.BlockSpec(memory_space=pltpu.SMEM)
    vmem = pl.BlockSpec(memory_space=pltpu.VMEM)
    hbm = pl.BlockSpec(memory_space=pl.ANY)
    return pl.pallas_call(
        functools.partial(crossed_kernel, rows),
        out_shape=[
            jax.ShapeDtypeStruct((b, b), F32),
            jax.ShapeDtypeStruct((16, 8, b // 16, b), BF),
        ],
        in_specs=[smem, smem, vmem, vmem, vmem] + [hbm] * 8,
        out_specs=[vmem] * 2,
        scratch_shapes=[
            pltpu.VMEM((8, rows + b, b), BF),
            pltpu.SemaphoreType.DMA((8, 2)),
        ],
        cost_estimate=pl.CostEstimate(
            flops=2 * rows * b * 8 * b, bytes_accessed=5_000_000, transcendentals=0
        ),
        compiler_params=pltpu.CompilerParams(vmem_limit_bytes=60 * 1024 * 1024),
        name="crossed",
    )(scal, parent, x, up, d_up, *cols)


def after(value, *others):
    return lax.optimization_barrier((value,) + others)[0]


def solution(mesh):
    def body(a, l_up, m_up, d_up, l_lo, m_lo, parent, lp, d_lo):
        rows, b = l_up.shape
        blocks = rows // b
        piece = b // 16
        g, row, col = lax.axis_index("grp"), lax.axis_index("row"), lax.axis_index("col")
        z, h = row // 2, row % 2
        v, x = col // 4, col % 4
        place = g * 8 + row

        def masked(factor, pattern):
            keep = lax.dynamic_slice(pattern, (col, place * blocks), (1, blocks)) > 0
            shaped = factor.reshape(blocks, b, b)
            return jnp.where(keep.reshape(blocks, 1, 1), shaped, jnp.zeros((), BF)).reshape(rows, b)

        up, lo = masked(l_up, m_up), masked(l_lo, m_lo)
        a_across = send(a, CORE)
        scal = jnp.stack([h, (-x - z) % 4, col, v, x, g, place]).astype(jnp.int32)

        def spread(k0, direct):
            o0 = send(k0, Y_HI)
            k3 = send(k0, Z_UP)
            k1 = send(k0, Z_DOWN)
            o3 = send(o0, Z_UP)
            o1 = send(o0, Z_DOWN)
            k2 = send(k0, Z_FAR) if direct else send(k3, Z_UP)
            o2 = send(o0, Z_FAR) if direct else send(o1, Z_DOWN)
            return k0, k1, k2, k3, o0, o1, o2, o3

        def reduce(parts):
            plus, minus, later_plus, later_minus, keep = parts
            r1 = send(plus, X_UP)
            r3 = send(minus, X_DOWN)
            s1 = (later_plus.astype(F32) + r1[:rows].astype(F32)).astype(BF)
            s3 = (later_minus.astype(F32) + r3[rows:].astype(F32)).astype(BF)
            q1 = send(s1, X_UP)
            q3 = send(s3, X_DOWN)
            mine = keep[:rows].astype(F32) + r3[:rows].astype(F32) + q1.astype(F32)
            other = keep[rows:].astype(F32) + r1[rows:].astype(F32) + q3.astype(F32)
            same = g == v
            first = jnp.where(same, other, mine).astype(BF)
            second = jnp.where(same, mine, other).astype(BF)
            first = send(first, LAST_A)
            second = send(second, LAST_B)
            return (-(first.astype(F32) + second.astype(F32))).astype(BF)

        up_pieces = spread(send(up, TURN), False)
        lo_first = send(after(lo, up_pieces[2]), TURN)

        own_col = jnp.concatenate([lo, lp, send(lp, Y_LO)], 0)
        own_col = after(own_col, up_pieces[0])
        far = send(lo, Y_LO)
        n1, f1 = send(own_col, X_DOWN), send(far, X_DOWN)
        n2, f2 = send(own_col, X_FAR), send(far, X_FAR)
        n3, f3 = send(own_col, X_UP), send(far, X_UP)
        near_cols = (own_col, n1, n2, n3)
        cols = near_cols + (far, f1, f2, f3)

        parts = products(scal, a, a_across, up_pieces)
        lo_pieces = spread(after(lo_first, parts[0]), True)
        x_own = reduce(parts)
        lo_parts = products(scal, a, a_across, lo_pieces)
        x_across = send(x_own, CORE)

        parts = couple(scal, parent, lo_parts, x_own, x_across, near_cols)
        y_own = reduce(parts)

        def halved(value):
            size = b // 2
            given = lax.dynamic_slice(value, ((1 - g) * size, 0), (size, b)).astype(BF)
            kept = lax.dynamic_slice(value, (g * size, 0), (size, b))
            return kept + send(given, CORE).astype(F32)

        upper, terms = crossed(scal, parent, x_own, up, d_up, cols)
        terms = lax.all_to_all(terms.reshape(128, piece, b), ALL, 0, 0, tiled=True)
        p_slice = (-jnp.sum(terms.astype(F32), 0)).astype(BF)

        half = b // 2
        diag = halved(upper).astype(BF)
        diag = lax.all_to_all(jnp.broadcast_to(after(diag, p_slice)[None], (8, half, b)), "row", 0, 0, tiled=True)
        d_half = lax.dynamic_slice(d_up, (g * half, 0), (half, b)) - jnp.sum(diag.astype(F32), 0)

        lp_slice = lax.dynamic_slice(lp, (place * piece, 0), (piece, b))
        own = dot(lo, y_own, (0, 0)) + dot(lp_slice, p_slice, (0, 0))
        own = halved(own).astype(BF)
        own = jnp.concatenate([own, p_slice], 0)
        own = lax.all_to_all(jnp.broadcast_to(own[None], (8,) + own.shape), "row", 0, 0, tiled=True)
        last = lax.dynamic_slice(d_lo, (g * half, 0), (half, b)) - jnp.sum(
            own[:, :half].astype(F32), 0
        )
        y_parent = own[:, half:].reshape(half, b)
        mine = jnp.concatenate([d_half.astype(BF), y_parent, last.astype(BF)], 1)
        other = send(mine, CORE)

        def whole(part):
            ours, theirs = mine[:, part * b : (part + 1) * b], other[:, part * b : (part + 1) * b]
            return jnp.where(
                g == 0, jnp.concatenate([ours, theirs], 0), jnp.concatenate([theirs, ours], 0)
            )

        return x_own, whole(0), y_own, whole(1), whole(2)

    tall, flat, full = P(GR, "col"), P(None, "col"), P(None, None)
    return jax.shard_map(
        body,
        mesh=mesh,
        in_specs=(tall, tall, full, flat, tall, full, P(None), flat, flat),
        out_specs=(tall, flat, tall, flat, flat),
        check_vma=False,
    )
```

```python
import functools

import jax
import jax.numpy as jnp
import numpy as np
from jax import lax
from jax.experimental import pallas as pl
from jax.experimental.pallas import tpu as pltpu
from jax.sharding import PartitionSpec as P


ALL = ("grp", "row", "col")
GR = ("grp", "row")
SHAPE = (2, 4, 2, 2, 4)
BF = jnp.bfloat16
F32 = jnp.float32


def perm(move):
    pairs = []
    for place in np.ndindex(*SHAPE):
        target = move(*place)
        pairs.append(
            (int(np.ravel_multi_index(place, SHAPE)), int(np.ravel_multi_index(target, SHAPE)))
        )
    return pairs


TURN = perm(lambda g, z, h, v, x: (v, -x % 4, h, g, z))
CORE = perm(lambda g, z, h, v, x: (1 - g, z, h, v, x))
Y_HI = perm(lambda g, z, h, v, x: (g, z, 1 - h, v, x))
Y_LO = perm(lambda g, z, h, v, x: (g, z, h, 1 - v, x))
Z_UP = perm(lambda g, z, h, v, x: (g, (z + 1) % 4, h, v, x))
Z_DOWN = perm(lambda g, z, h, v, x: (g, (z - 1) % 4, h, v, x))
X_FAR = perm(lambda g, z, h, v, x: (g, z, h, v, (x + 2) % 4))
Z_FAR = perm(lambda g, z, h, v, x: (g, (z + 2) % 4, h, v, x))
X_UP = perm(lambda g, z, h, v, x: (g, z, h, v, (x + 1) % 4))
X_DOWN = perm(lambda g, z, h, v, x: (g, z, h, v, (x - 1) % 4))
LAST_A = perm(lambda g, z, h, v, x: (1 - g, z, h, v, x) if g == v else (g, z, h, 1 - v, x))
LAST_B = perm(lambda g, z, h, v, x: (g, z, h, v, x) if g == v else (1 - g, z, h, 1 - v, x))


def send(value, pairs):
    return lax.ppermute(value, ALL, pairs)


def dot(a, b, contract):
    return lax.dot_general(a, b, ((contract[:1], contract[1:]), ((), ())), preferred_element_type=F32)


def targets_of(rows):
    own, across = pl.ds(0, rows), pl.ds(rows, rows)
    return (
        (2, 0, 0, own),
        (3, 0, 3, own),
        (1, 0, 4, own),
        (0, 0, 6, own),
        (2, 1, 1, own),
        (1, 1, 2, own),
        (3, 1, 5, own),
        (0, 1, 6, across),
    )


def shapes_of(rows, b):
    short = jax.ShapeDtypeStruct((rows, b), BF)
    return [short] * 6 + [jax.ShapeDtypeStruct((2 * rows, b), BF)]


CHUNKS = 3


def products_kernel(depth, rows, scal, *refs):
    pieces = refs[2:10]
    outs = refs[10:17]
    a_s, b_s, c_s, a_sems, b_sems, c_sems = refs[17:]
    half, offset = scal[0], scal[1]
    size = rows // CHUNKS
    b = c_s.shape[2]

    def a_copy(chunk, part):
        which = half if part == 0 else 1 - half
        block, step = divmod(chunk, CHUNKS)
        return pltpu.make_async_copy(
            refs[block].at[
                pl.ds(step * size, size), pl.ds(pl.multiple_of(which * depth, depth), depth)
            ],
            a_s.at[pl.ds(chunk * size, size), pl.ds(part * depth, depth)],
            a_sems.at[chunk, part],
        )

    def b_copy(piece, slot, part):
        return pltpu.make_async_copy(
            pieces[piece],
            b_s.at[pl.ds(part * depth, depth), pl.ds(pl.multiple_of(slot * b, b), b)],
            b_sems.at[slot, part],
        )

    for part in range(2):
        a_copy(0, part).start()
        for k in range(4):
            b_copy(part * 4 + k, lax.rem(offset - k + 4, 4), part).start()
    for j in range(4):
        b_copy(0, j, 0).wait()
        b_copy(0, j, 1).wait()
    for chunk in range(1, 3):
        a_copy(chunk, 0).start()
        a_copy(chunk, 1).start()
    copies = []
    for chunk in range(2 * CHUNKS):
        a_copy(chunk, 0).wait()
        a_copy(chunk, 1).wait()
        if chunk + 3 < 2 * CHUNKS:
            a_copy(chunk + 3, 0).start()
            a_copy(chunk + 3, 1).start()
        block, step = divmod(chunk, CHUNKS)
        total = jnp.dot(
            a_s[pl.ds(chunk * size, size), :], b_s[...], preferred_element_type=F32
        ).astype(BF)
        for n, (j, where, out, place) in enumerate(targets_of(rows)):
            if where == block:
                c_s[n, pl.ds(step * size, size), :] = total[:, j * b : (j + 1) * b]
                copies.append(
                    pltpu.make_async_copy(
                        c_s.at[n, pl.ds(step * size, size), :],
                        outs[out].at[pl.ds(place.start + step * size, size), :],
                        c_sems.at[n, step],
                    )
                )
                copies[-1].start()
    for copy in copies:
        copy.wait()


def products(scal, a, a_across, pieces):
    rows, width = a.shape
    depth, b = pieces[0].shape
    hbm = pl.BlockSpec(memory_space=pl.ANY)
    return pl.pallas_call(
        functools.partial(products_kernel, depth, rows),
        out_shape=shapes_of(rows, b),
        in_specs=[pl.BlockSpec(memory_space=pltpu.SMEM)] + [hbm] * 10,
        out_specs=[hbm] * 7,
        scratch_shapes=[
            pltpu.VMEM((2 * rows, width), BF),
            pltpu.VMEM((width, 4 * b), BF),
            pltpu.VMEM((8, rows, b), BF),
            pltpu.SemaphoreType.DMA((2 * CHUNKS, 2)),
            pltpu.SemaphoreType.DMA((4, 2)),
            pltpu.SemaphoreType.DMA((8, CHUNKS)),
        ],
        cost_estimate=pl.CostEstimate(
            flops=2 * 2 * rows * width * 4 * b, bytes_accessed=12_000_000, transcendentals=0
        ),
        compiler_params=pltpu.CompilerParams(vmem_limit_bytes=60 * 1024 * 1024),
        name="products",
    )(scal, a, a_across, *pieces)


def panel_at(n, rows):
    return n, 0, 0, rows


def link_at(n, rows, b):
    return n % 4, rows + n // 4 * b, rows, b


def couple_kernel(rows, scal, parent, x_own, x_across, *refs):
    cols, outs = refs[:4], refs[11:18]
    blocks, links, in_sems, out_sems, link_sems = refs[18:]
    col, v, x, g = scal[2], scal[3], scal[4], scal[5]
    b = links.shape[1]

    def used(j):
        return parent[4 * g + lax.rem(x + j, 4)] == col

    def block_in(n, out, place):
        return pltpu.make_async_copy(outs[out].at[place, :], blocks.at[n], in_sems.at[n])

    def block_out(n, out, place):
        return pltpu.make_async_copy(blocks.at[n], outs[out].at[place, :], out_sems.at[n])

    def link_in(j, far):
        buffer, start, _, size = link_at(j + 4 * far, rows, b)
        return pltpu.make_async_copy(
            cols[buffer].at[pl.ds(start, size), :], links.at[j], link_sems.at[j]
        )

    for j in range(4):
        for far in range(2):

            @pl.when(jnp.logical_and(used(j), (g == v) == (far == 0)))
            def _():
                link_in(j, far).start()

    for n, (j, block, out, place) in enumerate(targets_of(rows)):

        @pl.when(used(j))
        def _():
            block_in(n, out, place).start()

    for n, (j, block, out, place) in enumerate(targets_of(rows)):

        @pl.when(used(j))
        def _():
            if block == 0:
                link_in(j, 0).wait()
            block_in(n, out, place).wait()
            value = (x_own, x_across)[block]
            total = jnp.dot(value[...], links[j], preferred_element_type=F32)
            blocks[n] = (blocks[n].astype(F32) + total).astype(BF)
            block_out(n, out, place).start()

    for n, (j, block, out, place) in enumerate(targets_of(rows)):

        @pl.when(used(j))
        def _():
            block_out(n, out, place).wait()


def couple(scal, parent, parts, x_own, x_across, cols):
    rows, b = x_own.shape
    smem = pl.BlockSpec(memory_space=pltpu.SMEM)
    vmem = pl.BlockSpec(memory_space=pltpu.VMEM)
    hbm = pl.BlockSpec(memory_space=pl.ANY)
    return pl.pallas_call(
        functools.partial(couple_kernel, rows),
        out_shape=[jax.ShapeDtypeStruct(p.shape, BF) for p in parts],
        in_specs=[smem, smem, vmem, vmem] + [hbm] * 11,
        out_specs=[hbm] * 7,
        scratch_shapes=[
            pltpu.VMEM((8, rows, b), BF),
            pltpu.VMEM((4, b, b), BF),
            pltpu.SemaphoreType.DMA((8,)),
            pltpu.SemaphoreType.DMA((8,)),
            pltpu.SemaphoreType.DMA((4,)),
        ],
        input_output_aliases={8 + n: n for n in range(7)},
        cost_estimate=pl.CostEstimate(
            flops=2 * 2 * rows * b * 4 * b, bytes_accessed=8_000_000, transcendentals=0
        ),
        compiler_params=pltpu.CompilerParams(vmem_limit_bytes=60 * 1024 * 1024),
        name="couple",
    )(scal, parent, x_own, x_across, *cols, *parts)


def crossed_kernel(rows, scal, parent, x_ref, up_ref, d_ref, *refs):
    cols, (upper, terms, held, sems) = refs[:8], refs[8:]
    col, v, x, place = scal[2], scal[3], scal[4], scal[6]
    slices, _, piece, b = terms.shape

    def child(n):
        side = v if n < 4 else 1 - v
        return 4 * side + lax.rem(x + n % 4, 4)

    def fetch(n):
        parts = (panel_at(n, rows), link_at(n, rows, b))
        return [
            pltpu.make_async_copy(
                cols[source].at[pl.ds(start, size), :],
                held.at[n, pl.ds(to, size), :],
                sems.at[n, m],
            )
            for m, (source, start, to, size) in enumerate(parts)
        ]

    for n in range(8):

        @pl.when(parent[child(n)] == col)
        def _():
            for copy in fetch(n):
                copy.start()

    total = dot(up_ref[...], x_ref[...], (0, 0))
    upper[...] = total
    first = jnp.where(place == 0, 1.0, 0.0)
    diag = (d_ref[...] * first - total).astype(BF)
    for n in range(8):
        l = child(n)

        @pl.when(parent[l] == col)
        def _():
            for copy in fetch(n):
                copy.wait()
            term = dot(x_ref[...], held[n, pl.ds(0, rows), :], (0, 0))
            term += dot(diag, held[n, pl.ds(rows, b), :], (1, 0))
            terms[:, l] = term.astype(BF).reshape(slices, piece, b)

        @pl.when(parent[l] != col)
        def _():
            terms[:, l] = jnp.zeros((slices, piece, b), BF)


def crossed(scal, parent, x, up, d_up, cols):
    rows, b = x.shape
    smem = pl.BlockSpec(memory_space=pltpu.SMEM)
    vmem = pl.BlockSpec(memory_space=pltpu.VMEM)
    hbm = pl.BlockSpec(memory_space=pl.ANY)
    return pl.pallas_call(
        functools.partial(crossed_kernel, rows),
        out_shape=[
            jax.ShapeDtypeStruct((b, b), F32),
            jax.ShapeDtypeStruct((16, 8, b // 16, b), BF),
        ],
        in_specs=[smem, smem, vmem, vmem, vmem] + [hbm] * 8,
        out_specs=[vmem] * 2,
        scratch_shapes=[
            pltpu.VMEM((8, rows + b, b), BF),
            pltpu.SemaphoreType.DMA((8, 2)),
        ],
        cost_estimate=pl.CostEstimate(
            flops=2 * rows * b * 8 * b, bytes_accessed=5_000_000, transcendentals=0
        ),
        compiler_params=pltpu.CompilerParams(vmem_limit_bytes=60 * 1024 * 1024),
        name="crossed",
    )(scal, parent, x, up, d_up, *cols)


def after(value, *others):
    return lax.optimization_barrier((value,) + others)[0]


def solution(mesh):
    def body(a, l_up, m_up, d_up, l_lo, m_lo, parent, lp, d_lo):
        rows, b = l_up.shape
        blocks = rows // b
        piece = b // 16
        g, row, col = lax.axis_index("grp"), lax.axis_index("row"), lax.axis_index("col")
        z, h = row // 2, row % 2
        v, x = col // 4, col % 4
        place = g * 8 + row

        lp_slice = lax.optimization_barrier(lax.dynamic_slice(lp, (place * piece, 0), (piece, b)))

        def masked(factor, pattern):
            keep = lax.dynamic_slice(pattern, (col, place * blocks), (1, blocks)) > 0
            shaped = factor.reshape(blocks, b, b)
            return jnp.where(keep.reshape(blocks, 1, 1), shaped, jnp.zeros((), BF)).reshape(rows, b)

        up, lo = masked(l_up, m_up), masked(l_lo, m_lo)
        a_across = send(a, CORE)
        scal = jnp.stack([h, (-x - z) % 4, col, v, x, g, place]).astype(jnp.int32)

        def spread(k0, direct):
            o0 = send(k0, Y_HI)
            k3 = send(k0, Z_UP)
            k1 = send(k0, Z_DOWN)
            o3 = send(o0, Z_UP)
            o1 = send(o0, Z_DOWN)
            k2 = send(k3, Z_UP)
            o2 = send(o0, Z_FAR) if direct else send(o1, Z_DOWN)
            return k0, k1, k2, k3, o0, o1, o2, o3

        def reduce(parts):
            far_up, far_down, near_up, near_down, last_up, last_down, keep = parts
            far_up = send(far_up, X_UP)
            far_down = send(far_down, X_DOWN)
            near_up = send(near_up, X_UP)
            near_down = send(near_down, X_DOWN)
            last_up = (last_up.astype(F32) + far_up.astype(F32)).astype(BF)
            last_down = (last_down.astype(F32) + far_down.astype(F32)).astype(BF)
            last_up = send(last_up, X_UP)
            last_down = send(last_down, X_DOWN)
            mine = keep[:rows].astype(F32) + near_down.astype(F32) + last_up.astype(F32)
            other = keep[rows:].astype(F32) + near_up.astype(F32) + last_down.astype(F32)
            same = g == v
            first = jnp.where(same, other, mine).astype(BF)
            second = jnp.where(same, mine, other).astype(BF)
            first = send(first, LAST_A)
            second = send(second, LAST_B)
            return (-(first.astype(F32) + second.astype(F32))).astype(BF)

        up_pieces = spread(send(up, TURN), False)
        lo_first = send(after(lo, up_pieces[2]), TURN)

        own_col = jnp.concatenate([lo, lp, send(lp, Y_LO)], 0)
        own_col = after(own_col, up_pieces[0])
        far = send(lo, Y_LO)
        n1, f1 = send(own_col, X_DOWN), send(far, X_DOWN)
        n2, f2 = send(own_col, X_FAR), send(far, X_FAR)
        n3, f3 = send(own_col, X_UP), send(far, X_UP)
        near_cols = (own_col, n1, n2, n3)
        cols = near_cols + (far, f1, f2, f3)

        parts = products(scal, a, a_across, up_pieces)
        lo_pieces = spread(after(lo_first, parts[0]), True)
        x_own = reduce(parts)
        lo_parts = products(scal, a, a_across, lo_pieces)
        x_across = send(x_own, CORE)

        parts = couple(scal, parent, lo_parts, x_own, x_across, near_cols)
        y_own = reduce(parts)

        def halved(value):
            size, width = b // 2, value.shape[1]
            given = lax.dynamic_slice(value, ((1 - g) * size, 0), (size, width)).astype(BF)
            kept = lax.dynamic_slice(value, (g * size, 0), (size, width))
            return kept + send(given, CORE).astype(F32)

        upper, terms = crossed(scal, parent, x_own, up, d_up, cols)
        terms = lax.all_to_all(terms.reshape(128, piece, b), ALL, 0, 0, tiled=True)
        p_slice = (-jnp.sum(terms.astype(F32), 0)).astype(BF)

        half = b // 2
        own = dot(lo, y_own, (0, 0)) + dot(lp_slice, p_slice, (0, 0))
        own = halved(jnp.concatenate([own, upper], 1)).astype(BF)
        own = jnp.concatenate([own[:, :b], own[:, b:], p_slice], 0)
        own = lax.all_to_all(jnp.broadcast_to(own[None], (8,) + own.shape), "row", 0, 0, tiled=True)
        sums = jnp.sum(own[:, :b].astype(F32), 0)
        d_half = lax.dynamic_slice(d_up, (g * half, 0), (half, b)) - sums[half:]
        last = lax.dynamic_slice(d_lo, (g * half, 0), (half, b)) - sums[:half]
        y_parent = own[:, b:].reshape(half, b)
        mine = jnp.concatenate([d_half.astype(BF), y_parent, last.astype(BF)], 1)
        other = send(mine, CORE)

        def whole(part):
            ours, theirs = mine[:, part * b : (part + 1) * b], other[:, part * b : (part + 1) * b]
            return jnp.where(
                g == 0, jnp.concatenate([ours, theirs], 0), jnp.concatenate([theirs, ours], 0)
            )

        return x_own, whole(0), y_own, whole(1), whole(2)

    tall, flat, full = P(GR, "col"), P(None, "col"), P(None, None)
    return jax.shard_map(
        body,
        mesh=mesh,
        in_specs=(tall, tall, full, flat, tall, full, P(None), flat, flat),
        out_specs=(tall, flat, tall, flat, flat),
        check_vma=False,
    )
```

```python
import functools

import jax
import jax.numpy as jnp
import numpy as np
from jax import lax
from jax.experimental import pallas as pl
from jax.experimental.pallas import tpu as pltpu
from jax.sharding import PartitionSpec as P


ALL = ("grp", "row", "col")
GR = ("grp", "row")
SHAPE = (2, 4, 2, 2, 4)
BF = jnp.bfloat16
F32 = jnp.float32


def perm(move):
    pairs = []
    for place in np.ndindex(*SHAPE):
        target = move(*place)
        pairs.append(
            (int(np.ravel_multi_index(place, SHAPE)), int(np.ravel_multi_index(target, SHAPE)))
        )
    return pairs


TURN = perm(lambda g, z, h, v, x: (v, -x % 4, h, g, z))
CORE = perm(lambda g, z, h, v, x: (1 - g, z, h, v, x))
Y_HI = perm(lambda g, z, h, v, x: (g, z, 1 - h, v, x))
Y_LO = perm(lambda g, z, h, v, x: (g, z, h, 1 - v, x))
Z_UP = perm(lambda g, z, h, v, x: (g, (z + 1) % 4, h, v, x))
Z_DOWN = perm(lambda g, z, h, v, x: (g, (z - 1) % 4, h, v, x))
X_FAR = perm(lambda g, z, h, v, x: (g, z, h, v, (x + 2) % 4))
X_UP = perm(lambda g, z, h, v, x: (g, z, h, v, (x + 1) % 4))
X_DOWN = perm(lambda g, z, h, v, x: (g, z, h, v, (x - 1) % 4))
LAST_A = perm(lambda g, z, h, v, x: (1 - g, z, h, v, x) if g == v else (g, z, h, 1 - v, x))
LAST_B = perm(lambda g, z, h, v, x: (g, z, h, v, x) if g == v else (1 - g, z, h, 1 - v, x))


def send(value, pairs):
    return lax.ppermute(value, ALL, pairs)


def dot(a, b, contract):
    return lax.dot_general(a, b, ((contract[:1], contract[1:]), ((), ())), preferred_element_type=F32)


def targets_of(rows):
    own, across = pl.ds(0, rows), pl.ds(rows, rows)
    return (
        (2, 0, 0, own),
        (3, 0, 3, own),
        (1, 0, 4, own),
        (0, 0, 6, own),
        (2, 1, 1, own),
        (1, 1, 2, own),
        (3, 1, 5, own),
        (0, 1, 6, across),
    )


def shapes_of(rows, b):
    short = jax.ShapeDtypeStruct((rows, b), BF)
    return [short] * 6 + [jax.ShapeDtypeStruct((2 * rows, b), BF)]


CHUNKS = 3


def products_kernel(depth, rows, scal, *refs):
    pieces = refs[2:10]
    outs = refs[10:17]
    a_s, b_s, c_s, a_sems, b_sems, c_sems = refs[17:]
    half, offset = scal[0], scal[1]
    size = rows // CHUNKS
    b = c_s.shape[2]

    def a_copy(chunk, part):
        which = half if part == 0 else 1 - half
        block, step = divmod(chunk, CHUNKS)
        return pltpu.make_async_copy(
            refs[block].at[
                pl.ds(step * size, size), pl.ds(pl.multiple_of(which * depth, depth), depth)
            ],
            a_s.at[pl.ds(chunk * size, size), pl.ds(part * depth, depth)],
            a_sems.at[chunk, part],
        )

    def b_copy(piece, slot, part):
        return pltpu.make_async_copy(
            pieces[piece],
            b_s.at[pl.ds(part * depth, depth), pl.ds(pl.multiple_of(slot * b, b), b)],
            b_sems.at[slot, part],
        )

    for part in range(2):
        a_copy(0, part).start()
        for k in range(4):
            b_copy(part * 4 + k, lax.rem(offset - k + 4, 4), part).start()
    for j in range(4):
        b_copy(0, j, 0).wait()
        b_copy(0, j, 1).wait()
    for chunk in range(1, 3):
        a_copy(chunk, 0).start()
        a_copy(chunk, 1).start()
    copies = []
    for chunk in range(2 * CHUNKS):
        a_copy(chunk, 0).wait()
        a_copy(chunk, 1).wait()
        if chunk + 3 < 2 * CHUNKS:
            a_copy(chunk + 3, 0).start()
            a_copy(chunk + 3, 1).start()
        block, step = divmod(chunk, CHUNKS)
        total = jnp.dot(
            a_s[pl.ds(chunk * size, size), :], b_s[...], preferred_element_type=F32
        ).astype(BF)
        for n, (j, where, out, place) in enumerate(targets_of(rows)):
            if where == block:
                c_s[n, pl.ds(step * size, size), :] = total[:, j * b : (j + 1) * b]
                copies.append(
                    pltpu.make_async_copy(
                        c_s.at[n, pl.ds(step * size, size), :],
                        outs[out].at[pl.ds(place.start + step * size, size), :],
                        c_sems.at[n, step],
                    )
                )
                copies[-1].start()
    for copy in copies:
        copy.wait()


def products(scal, a, a_across, pieces):
    rows, width = a.shape
    depth, b = pieces[0].shape
    hbm = pl.BlockSpec(memory_space=pl.ANY)
    return pl.pallas_call(
        functools.partial(products_kernel, depth, rows),
        out_shape=shapes_of(rows, b),
        in_specs=[pl.BlockSpec(memory_space=pltpu.SMEM)] + [hbm] * 10,
        out_specs=[hbm] * 7,
        scratch_shapes=[
            pltpu.VMEM((2 * rows, width), BF),
            pltpu.VMEM((width, 4 * b), BF),
            pltpu.VMEM((8, rows, b), BF),
            pltpu.SemaphoreType.DMA((2 * CHUNKS, 2)),
            pltpu.SemaphoreType.DMA((4, 2)),
            pltpu.SemaphoreType.DMA((8, CHUNKS)),
        ],
        cost_estimate=pl.CostEstimate(
            flops=2 * 2 * rows * width * 4 * b, bytes_accessed=12_000_000, transcendentals=0
        ),
        compiler_params=pltpu.CompilerParams(vmem_limit_bytes=60 * 1024 * 1024),
        name="products",
    )(scal, a, a_across, *pieces)


def panel_at(n, rows):
    return n, 0, 0, rows


def link_at(n, rows, b):
    return n % 4, rows + n // 4 * b, rows, b


def couple_kernel(rows, scal, parent, x_own, x_across, *refs):
    cols, outs = refs[:4], refs[11:18]
    blocks, links, in_sems, out_sems, link_sems = refs[18:]
    col, v, x, g = scal[2], scal[3], scal[4], scal[5]
    b = links.shape[1]

    def used(j):
        return parent[4 * g + lax.rem(x + j, 4)] == col

    def block_in(n, out, place):
        return pltpu.make_async_copy(outs[out].at[place, :], blocks.at[n], in_sems.at[n])

    def block_out(n, out, place):
        return pltpu.make_async_copy(blocks.at[n], outs[out].at[place, :], out_sems.at[n])

    def link_in(j, far):
        buffer, start, _, size = link_at(j + 4 * far, rows, b)
        return pltpu.make_async_copy(
            cols[buffer].at[pl.ds(start, size), :], links.at[j], link_sems.at[j]
        )

    for j in range(4):
        for far in range(2):

            @pl.when(jnp.logical_and(used(j), (g == v) == (far == 0)))
            def _():
                link_in(j, far).start()

    for n, (j, block, out, place) in enumerate(targets_of(rows)):

        @pl.when(used(j))
        def _():
            block_in(n, out, place).start()

    for n, (j, block, out, place) in enumerate(targets_of(rows)):

        @pl.when(used(j))
        def _():
            if block == 0:
                link_in(j, 0).wait()
            block_in(n, out, place).wait()
            value = (x_own, x_across)[block]
            total = jnp.dot(value[...], links[j], preferred_element_type=F32)
            blocks[n] = (blocks[n].astype(F32) + total).astype(BF)
            block_out(n, out, place).start()

    for n, (j, block, out, place) in enumerate(targets_of(rows)):

        @pl.when(used(j))
        def _():
            block_out(n, out, place).wait()


def couple(scal, parent, parts, x_own, x_across, cols):
    rows, b = x_own.shape
    smem = pl.BlockSpec(memory_space=pltpu.SMEM)
    vmem = pl.BlockSpec(memory_space=pltpu.VMEM)
    hbm = pl.BlockSpec(memory_space=pl.ANY)
    return pl.pallas_call(
        functools.partial(couple_kernel, rows),
        out_shape=[jax.ShapeDtypeStruct(p.shape, BF) for p in parts],
        in_specs=[smem, smem, vmem, vmem] + [hbm] * 11,
        out_specs=[hbm] * 7,
        scratch_shapes=[
            pltpu.VMEM((8, rows, b), BF),
            pltpu.VMEM((4, b, b), BF),
            pltpu.SemaphoreType.DMA((8,)),
            pltpu.SemaphoreType.DMA((8,)),
            pltpu.SemaphoreType.DMA((4,)),
        ],
        input_output_aliases={8 + n: n for n in range(7)},
        cost_estimate=pl.CostEstimate(
            flops=2 * 2 * rows * b * 4 * b, bytes_accessed=8_000_000, transcendentals=0
        ),
        compiler_params=pltpu.CompilerParams(vmem_limit_bytes=60 * 1024 * 1024),
        name="couple",
    )(scal, parent, x_own, x_across, *cols, *parts)


def crossed_kernel(rows, scal, parent, x_ref, up_ref, d_ref, *refs):
    cols, outs, (held, whole, sems) = refs[:8], refs[8:12], refs[12:]
    upper_kept, upper_given, kept, given = outs
    col, v, x, g, place = scal[2], scal[3], scal[4], scal[5], scal[6]
    slices, _, piece, b = kept.shape
    half = b // 2
    ours = pl.ds(pl.multiple_of(g * half, half), half)
    theirs = pl.ds(pl.multiple_of((1 - g) * half, half), half)

    def child(n):
        side = v if n < 4 else 1 - v
        return 4 * side + lax.rem(x + n % 4, 4)

    def fetch(n):
        parts = (panel_at(n, rows), link_at(n, rows, b))
        return [
            pltpu.make_async_copy(
                cols[source].at[pl.ds(start, size), :],
                held.at[n, pl.ds(to, size), :],
                sems.at[n, m],
            )
            for m, (source, start, to, size) in enumerate(parts)
        ]

    for n in range(8):

        @pl.when(parent[child(n)] == col)
        def _():
            for copy in fetch(n):
                copy.start()

    total = dot(up_ref[...], x_ref[...], (0, 0))
    whole[...] = total
    upper_kept[...] = whole[ours, :]
    upper_given[...] = whole[theirs, :].astype(BF)
    first = jnp.where(place == 0, 1.0, 0.0)
    diag = (d_ref[...] * first - total).astype(BF)
    for n in range(8):
        l = child(n)

        @pl.when(parent[l] == col)
        def _():
            for copy in fetch(n):
                copy.wait()
            term = dot(x_ref[...], held[n, pl.ds(0, rows), :], (0, 0))
            term += dot(diag, held[n, pl.ds(rows, b), :], (1, 0))
            whole[...] = term
            kept[:, l] = whole[ours, :].astype(BF).reshape(slices, piece, b)
            given[:, l] = whole[theirs, :].astype(BF).reshape(slices, piece, b)

        @pl.when(parent[l] != col)
        def _():
            kept[:, l] = jnp.zeros((slices, piece, b), BF)
            given[:, l] = jnp.zeros((slices, piece, b), BF)


def crossed(scal, parent, x, up, d_up, cols):
    rows, b = x.shape
    smem = pl.BlockSpec(memory_space=pltpu.SMEM)
    vmem = pl.BlockSpec(memory_space=pltpu.VMEM)
    hbm = pl.BlockSpec(memory_space=pl.ANY)
    return pl.pallas_call(
        functools.partial(crossed_kernel, rows),
        out_shape=[
            jax.ShapeDtypeStruct((b // 2, b), F32),
            jax.ShapeDtypeStruct((b // 2, b), BF),
            jax.ShapeDtypeStruct((8, 8, b // 16, b), BF),
            jax.ShapeDtypeStruct((8, 8, b // 16, b), BF),
        ],
        in_specs=[smem, smem, vmem, vmem, vmem] + [hbm] * 8,
        out_specs=[vmem] * 4,
        scratch_shapes=[
            pltpu.VMEM((8, rows + b, b), BF),
            pltpu.VMEM((b, b), F32),
            pltpu.SemaphoreType.DMA((8, 2)),
        ],
        cost_estimate=pl.CostEstimate(
            flops=2 * rows * b * 8 * b, bytes_accessed=5_000_000, transcendentals=0
        ),
        compiler_params=pltpu.CompilerParams(vmem_limit_bytes=60 * 1024 * 1024),
        name="crossed",
    )(scal, parent, x, up, d_up, *cols)


def after(value, *others):
    return lax.optimization_barrier((value,) + others)[0]


def solution(mesh):
    def body(a, l_up, m_up, d_up, l_lo, m_lo, parent, lp, d_lo):
        rows, b = l_up.shape
        blocks = rows // b
        piece = b // 16
        g, row, col = lax.axis_index("grp"), lax.axis_index("row"), lax.axis_index("col")
        z, h = row // 2, row % 2
        v, x = col // 4, col % 4
        place = g * 8 + row

        lp_slice = lax.optimization_barrier(lax.dynamic_slice(lp, (place * piece, 0), (piece, b)))

        def masked(factor, pattern):
            keep = lax.dynamic_slice(pattern, (col, place * blocks), (1, blocks)) > 0
            shaped = factor.reshape(blocks, b, b)
            return jnp.where(keep.reshape(blocks, 1, 1), shaped, jnp.zeros((), BF)).reshape(rows, b)

        up, lo = masked(l_up, m_up), masked(l_lo, m_lo)
        a_across = send(a, CORE)
        scal = jnp.stack([h, (-x - z) % 4, col, v, x, g, place]).astype(jnp.int32)

        def spread(k0):
            o0 = send(k0, Y_HI)
            k3 = send(k0, Z_UP)
            k1 = send(k0, Z_DOWN)
            o3 = send(o0, Z_UP)
            o1 = send(o0, Z_DOWN)
            k2 = send(k3, Z_UP)
            o2 = send(o1, Z_DOWN)
            return k0, k1, k2, k3, o0, o1, o2, o3

        def reduce(parts):
            far_up, far_down, near_up, near_down, last_up, last_down, keep = parts
            far_up = send(far_up, X_UP)
            far_down = send(far_down, X_DOWN)
            near_up = send(near_up, X_UP)
            near_down = send(near_down, X_DOWN)
            last_up = (last_up.astype(F32) + far_up.astype(F32)).astype(BF)
            last_down = (last_down.astype(F32) + far_down.astype(F32)).astype(BF)
            last_up = send(last_up, X_UP)
            last_down = send(last_down, X_DOWN)
            mine = keep[:rows].astype(F32) + near_down.astype(F32) + last_up.astype(F32)
            other = keep[rows:].astype(F32) + near_up.astype(F32) + last_down.astype(F32)
            same = g == v
            first = jnp.where(same, other, mine).astype(BF)
            second = jnp.where(same, mine, other).astype(BF)
            first = send(first, LAST_A)
            second = send(second, LAST_B)
            return (-(first.astype(F32) + second.astype(F32))).astype(BF)

        up_pieces = spread(send(up, TURN))
        lo_first = send(after(lo, up_pieces[2]), TURN)

        own_col = jnp.concatenate([lo, lp, send(lp, Y_LO)], 0)
        own_col = after(own_col, up_pieces[0])
        far = send(lo, Y_LO)
        n1, f1 = send(own_col, X_DOWN), send(far, X_DOWN)
        n2, f2 = send(own_col, X_FAR), send(far, X_FAR)
        n3, f3 = send(own_col, X_UP), send(far, X_UP)
        near_cols = (own_col, n1, n2, n3)
        cols = near_cols + (far, f1, f2, f3)

        parts = products(scal, a, a_across, up_pieces)
        lo_pieces = spread(after(lo_first, parts[0]))
        x_own = reduce(parts)
        lo_parts = products(scal, a, a_across, lo_pieces)
        x_across = send(x_own, CORE)

        parts = couple(scal, parent, lo_parts, x_own, x_across, near_cols)
        y_own = reduce(parts)

        upper, upper_given, kept, given = crossed(scal, parent, x_own, up, d_up, cols)
        terms = kept.astype(F32) + send(given, CORE).astype(F32)
        upper = upper + send(upper_given, CORE).astype(F32)
        terms = terms.astype(BF).reshape(64, piece, b)
        terms = lax.all_to_all(terms, ("row", "col"), 0, 0, tiled=True)
        p_slice = (-jnp.sum(terms.astype(F32), 0)).astype(BF)

        half = b // 2
        diag = after(upper.astype(BF), p_slice)
        diag = lax.all_to_all(jnp.broadcast_to(diag[None], (8, half, b)), "row", 0, 0, tiled=True)
        d_half = lax.dynamic_slice(d_up, (g * half, 0), (half, b)) - jnp.sum(diag.astype(F32), 0)

        own = dot(lo, y_own, (0, 0)) + dot(lp_slice, p_slice, (0, 0))
        own_given = lax.dynamic_slice(own, ((1 - g) * half, 0), (half, b)).astype(BF)
        own = lax.dynamic_slice(own, (g * half, 0), (half, b))
        own = (own + send(own_given, CORE).astype(F32)).astype(BF)
        own = jnp.concatenate([own, p_slice], 0)
        own = lax.all_to_all(jnp.broadcast_to(own[None], (8,) + own.shape), "row", 0, 0, tiled=True)
        last = lax.dynamic_slice(d_lo, (g * half, 0), (half, b)) - jnp.sum(
            own[:, :half].astype(F32), 0
        )
        y_parent = own[:, half:].reshape(half, b)
        mine = jnp.concatenate([d_half.astype(BF), y_parent, last.astype(BF)], 1)
        other = send(mine, CORE)

        def whole(part):
            ours, theirs = mine[:, part * b : (part + 1) * b], other[:, part * b : (part + 1) * b]
            return jnp.where(
                g == 0, jnp.concatenate([ours, theirs], 0), jnp.concatenate([theirs, ours], 0)
            )

        return x_own, whole(0), y_own, whole(1), whole(2)

    tall, flat, full = P(GR, "col"), P(None, "col"), P(None, None)
    return jax.shard_map(
        body,
        mesh=mesh,
        in_specs=(tall, tall, full, flat, tall, full, P(None), flat, flat),
        out_specs=(tall, flat, tall, flat, flat),
        check_vma=False,
    )
```

```python
import functools

import jax
import jax.numpy as jnp
import numpy as np
from jax import lax
from jax.experimental import pallas as pl
from jax.experimental.pallas import tpu as pltpu
from jax.sharding import PartitionSpec as P


ALL = ("grp", "row", "col")
GR = ("grp", "row")
SHAPE = (2, 4, 2, 2, 4)
BF = jnp.bfloat16
F32 = jnp.float32


def perm(move):
    pairs = []
    for place in np.ndindex(*SHAPE):
        target = move(*place)
        pairs.append(
            (int(np.ravel_multi_index(place, SHAPE)), int(np.ravel_multi_index(target, SHAPE)))
        )
    return pairs


TURN = perm(lambda g, z, h, v, x: (v, -x % 4, h, g, z))
CORE = perm(lambda g, z, h, v, x: (1 - g, z, h, v, x))
Y_HI = perm(lambda g, z, h, v, x: (g, z, 1 - h, v, x))
Y_LO = perm(lambda g, z, h, v, x: (g, z, h, 1 - v, x))
Z_UP = perm(lambda g, z, h, v, x: (g, (z + 1) % 4, h, v, x))
Z_DOWN = perm(lambda g, z, h, v, x: (g, (z - 1) % 4, h, v, x))
X_FAR = perm(lambda g, z, h, v, x: (g, z, h, v, (x + 2) % 4))
X_UP = perm(lambda g, z, h, v, x: (g, z, h, v, (x + 1) % 4))
X_DOWN = perm(lambda g, z, h, v, x: (g, z, h, v, (x - 1) % 4))
LAST_A = perm(lambda g, z, h, v, x: (1 - g, z, h, v, x) if g == v else (g, z, h, 1 - v, x))
LAST_B = perm(lambda g, z, h, v, x: (g, z, h, v, x) if g == v else (1 - g, z, h, 1 - v, x))


def send(value, pairs):
    return lax.ppermute(value, ALL, pairs)


def dot(a, b, contract):
    return lax.dot_general(a, b, ((contract[:1], contract[1:]), ((), ())), preferred_element_type=F32)


def targets_of(rows):
    own, across = pl.ds(0, rows), pl.ds(rows, rows)
    return (
        (2, 0, 0, own),
        (3, 0, 3, own),
        (1, 0, 4, own),
        (0, 0, 6, own),
        (2, 1, 1, own),
        (1, 1, 2, own),
        (3, 1, 5, own),
        (0, 1, 6, across),
    )


def shapes_of(rows, b):
    short = jax.ShapeDtypeStruct((rows, b), BF)
    return [short] * 6 + [jax.ShapeDtypeStruct((2 * rows, b), BF)]


CHUNKS = 3


def products_kernel(depth, rows, scal, *refs):
    pieces = refs[2:10]
    mask, outs = refs[10:-13], refs[-13:-6]
    a_s, b_s, c_s, a_sems, b_sems, c_sems = refs[-6:]
    half, offset = scal[0], scal[1]
    size = rows // CHUNKS
    b = c_s.shape[2]

    def a_copy(chunk, part):
        which = half if part == 0 else 1 - half
        block, step = divmod(chunk, CHUNKS)
        return pltpu.make_async_copy(
            refs[block].at[
                pl.ds(step * size, size), pl.ds(pl.multiple_of(which * depth, depth), depth)
            ],
            a_s.at[pl.ds(chunk * size, size), pl.ds(part * depth, depth)],
            a_sems.at[chunk, part],
        )

    def b_copy(piece, slot, part):
        return pltpu.make_async_copy(
            pieces[piece],
            b_s.at[pl.ds(part * depth, depth), pl.ds(pl.multiple_of(slot * b, b), b)],
            b_sems.at[slot, part],
        )

    for part in range(2):
        a_copy(0, part).start()
        for k in range(4):
            b_copy(part * 4 + k, lax.rem(offset - k + 4, 4), part).start()
    for j in range(4):
        b_copy(0, j, 0).wait()
        b_copy(0, j, 1).wait()
    for chunk in range(1, 3):
        a_copy(chunk, 0).start()
        a_copy(chunk, 1).start()
    for j in range(4 if mask else 0):
        u = 4 * scal[5] + lax.rem(scal[4] + j, 4)
        for part in range(2):
            which = half if part == 0 else 1 - half
            for n in range(depth // b):

                @pl.when(mask[0][u, (2 * scal[2] + which) * (depth // b) + n] <= 0)
                def _():
                    b_s[pl.ds(part * depth + n * b, b), pl.ds(j * b, b)] = jnp.zeros((b, b), BF)

    copies = []
    for chunk in range(2 * CHUNKS):
        a_copy(chunk, 0).wait()
        a_copy(chunk, 1).wait()
        if chunk + 3 < 2 * CHUNKS:
            a_copy(chunk + 3, 0).start()
            a_copy(chunk + 3, 1).start()
        block, step = divmod(chunk, CHUNKS)
        total = jnp.dot(
            a_s[pl.ds(chunk * size, size), :], b_s[...], preferred_element_type=F32
        ).astype(BF)
        for n, (j, where, out, place) in enumerate(targets_of(rows)):
            if where == block:
                c_s[n, pl.ds(step * size, size), :] = total[:, j * b : (j + 1) * b]
                copies.append(
                    pltpu.make_async_copy(
                        c_s.at[n, pl.ds(step * size, size), :],
                        outs[out].at[pl.ds(place.start + step * size, size), :],
                        c_sems.at[n, step],
                    )
                )
                copies[-1].start()
    for copy in copies:
        copy.wait()


def products(scal, a, a_across, pieces, mask=()):
    rows, width = a.shape
    depth, b = pieces[0].shape
    hbm = pl.BlockSpec(memory_space=pl.ANY)
    smem = pl.BlockSpec(memory_space=pltpu.SMEM)
    return pl.pallas_call(
        functools.partial(products_kernel, depth, rows),
        out_shape=shapes_of(rows, b),
        in_specs=[smem] + [hbm] * 10 + [smem] * len(mask),
        out_specs=[hbm] * 7,
        scratch_shapes=[
            pltpu.VMEM((2 * rows, width), BF),
            pltpu.VMEM((width, 4 * b), BF),
            pltpu.VMEM((8, rows, b), BF),
            pltpu.SemaphoreType.DMA((2 * CHUNKS, 2)),
            pltpu.SemaphoreType.DMA((4, 2)),
            pltpu.SemaphoreType.DMA((8, CHUNKS)),
        ],
        cost_estimate=pl.CostEstimate(
            flops=2 * 2 * rows * width * 4 * b, bytes_accessed=12_000_000, transcendentals=0
        ),
        compiler_params=pltpu.CompilerParams(vmem_limit_bytes=60 * 1024 * 1024),
        name="products",
    )(scal, a, a_across, *pieces, *mask)


def panel_at(n, rows):
    return n, 0, 0, rows


def link_at(n, rows, b):
    return n % 4, rows + n // 4 * b, rows, b


def couple_kernel(rows, scal, parent, x_own, x_across, *refs):
    cols, outs = refs[:4], refs[11:18]
    blocks, links, in_sems, out_sems, link_sems = refs[18:]
    col, v, x, g = scal[2], scal[3], scal[4], scal[5]
    b = links.shape[1]

    def used(j):
        return parent[4 * g + lax.rem(x + j, 4)] == col

    def block_in(n, out, place):
        return pltpu.make_async_copy(outs[out].at[place, :], blocks.at[n], in_sems.at[n])

    def block_out(n, out, place):
        return pltpu.make_async_copy(blocks.at[n], outs[out].at[place, :], out_sems.at[n])

    def link_in(j, far):
        buffer, start, _, size = link_at(j + 4 * far, rows, b)
        return pltpu.make_async_copy(
            cols[buffer].at[pl.ds(start, size), :], links.at[j], link_sems.at[j]
        )

    for j in range(4):
        for far in range(2):

            @pl.when(jnp.logical_and(used(j), (g == v) == (far == 0)))
            def _():
                link_in(j, far).start()

    for n, (j, block, out, place) in enumerate(targets_of(rows)):

        @pl.when(used(j))
        def _():
            block_in(n, out, place).start()

    for n, (j, block, out, place) in enumerate(targets_of(rows)):

        @pl.when(used(j))
        def _():
            if block == 0:
                link_in(j, 0).wait()
            block_in(n, out, place).wait()
            value = (x_own, x_across)[block]
            total = jnp.dot(value[...], links[j], preferred_element_type=F32)
            blocks[n] = (blocks[n].astype(F32) + total).astype(BF)
            block_out(n, out, place).start()

    for n, (j, block, out, place) in enumerate(targets_of(rows)):

        @pl.when(used(j))
        def _():
            block_out(n, out, place).wait()


def couple(scal, parent, parts, x_own, x_across, cols):
    rows, b = x_own.shape
    smem = pl.BlockSpec(memory_space=pltpu.SMEM)
    vmem = pl.BlockSpec(memory_space=pltpu.VMEM)
    hbm = pl.BlockSpec(memory_space=pl.ANY)
    return pl.pallas_call(
        functools.partial(couple_kernel, rows),
        out_shape=[jax.ShapeDtypeStruct(p.shape, BF) for p in parts],
        in_specs=[smem, smem, vmem, vmem] + [hbm] * 11,
        out_specs=[hbm] * 7,
        scratch_shapes=[
            pltpu.VMEM((8, rows, b), BF),
            pltpu.VMEM((4, b, b), BF),
            pltpu.SemaphoreType.DMA((8,)),
            pltpu.SemaphoreType.DMA((8,)),
            pltpu.SemaphoreType.DMA((4,)),
        ],
        input_output_aliases={8 + n: n for n in range(7)},
        cost_estimate=pl.CostEstimate(
            flops=2 * 2 * rows * b * 4 * b, bytes_accessed=8_000_000, transcendentals=0
        ),
        compiler_params=pltpu.CompilerParams(vmem_limit_bytes=60 * 1024 * 1024),
        name="couple",
    )(scal, parent, x_own, x_across, *cols, *parts)


def crossed_kernel(rows, scal, parent, x_ref, up_ref, d_ref, *refs):
    cols, outs, (held, whole, sems) = refs[:8], refs[8:12], refs[12:]
    upper_kept, upper_given, kept, given = outs
    col, v, x, g, place = scal[2], scal[3], scal[4], scal[5], scal[6]
    slices, _, piece, b = kept.shape
    half = b // 2
    ours = pl.ds(pl.multiple_of(g * half, half), half)
    theirs = pl.ds(pl.multiple_of((1 - g) * half, half), half)

    def child(n):
        side = v if n < 4 else 1 - v
        return 4 * side + lax.rem(x + n % 4, 4)

    def fetch(n):
        parts = (panel_at(n, rows), link_at(n, rows, b))
        return [
            pltpu.make_async_copy(
                cols[source].at[pl.ds(start, size), :],
                held.at[n, pl.ds(to, size), :],
                sems.at[n, m],
            )
            for m, (source, start, to, size) in enumerate(parts)
        ]

    for n in range(8):

        @pl.when(parent[child(n)] == col)
        def _():
            for copy in fetch(n):
                copy.start()

    total = dot(up_ref[...], x_ref[...], (0, 0))
    whole[...] = total
    upper_kept[...] = whole[ours, :]
    upper_given[...] = whole[theirs, :].astype(BF)
    first = jnp.where(place == 0, 1.0, 0.0)
    diag = (d_ref[...] * first - total).astype(BF)
    for n in range(8):
        l = child(n)

        @pl.when(parent[l] == col)
        def _():
            for copy in fetch(n):
                copy.wait()
            term = dot(x_ref[...], held[n, pl.ds(0, rows), :], (0, 0))
            term += dot(diag, held[n, pl.ds(rows, b), :], (1, 0))
            whole[...] = term
            kept[:, l] = whole[ours, :].astype(BF).reshape(slices, piece, b)
            given[:, l] = whole[theirs, :].astype(BF).reshape(slices, piece, b)

        @pl.when(parent[l] != col)
        def _():
            kept[:, l] = jnp.zeros((slices, piece, b), BF)
            given[:, l] = jnp.zeros((slices, piece, b), BF)


def crossed(scal, parent, x, up, d_up, cols):
    rows, b = x.shape
    smem = pl.BlockSpec(memory_space=pltpu.SMEM)
    vmem = pl.BlockSpec(memory_space=pltpu.VMEM)
    hbm = pl.BlockSpec(memory_space=pl.ANY)
    return pl.pallas_call(
        functools.partial(crossed_kernel, rows),
        out_shape=[
            jax.ShapeDtypeStruct((b // 2, b), F32),
            jax.ShapeDtypeStruct((b // 2, b), BF),
            jax.ShapeDtypeStruct((8, 8, b // 16, b), BF),
            jax.ShapeDtypeStruct((8, 8, b // 16, b), BF),
        ],
        in_specs=[smem, smem, vmem, vmem, vmem] + [hbm] * 8,
        out_specs=[vmem] * 4,
        scratch_shapes=[
            pltpu.VMEM((8, rows + b, b), BF),
            pltpu.VMEM((b, b), F32),
            pltpu.SemaphoreType.DMA((8, 2)),
        ],
        cost_estimate=pl.CostEstimate(
            flops=2 * rows * b * 8 * b, bytes_accessed=5_000_000, transcendentals=0
        ),
        compiler_params=pltpu.CompilerParams(vmem_limit_bytes=60 * 1024 * 1024),
        name="crossed",
    )(scal, parent, x, up, d_up, *cols)


def after(value, *others):
    return lax.optimization_barrier((value,) + others)[0]


def solution(mesh):
    def body(a, l_up, m_up, d_up, l_lo, m_lo, parent, lp, d_lo):
        rows, b = l_up.shape
        blocks = rows // b
        piece = b // 16
        g, row, col = lax.axis_index("grp"), lax.axis_index("row"), lax.axis_index("col")
        z, h = row // 2, row % 2
        v, x = col // 4, col % 4
        place = g * 8 + row

        lp_slice = lax.optimization_barrier(lax.dynamic_slice(lp, (place * piece, 0), (piece, b)))

        def masked(factor, pattern):
            keep = lax.dynamic_slice(pattern, (col, place * blocks), (1, blocks)) > 0
            shaped = factor.reshape(blocks, b, b)
            return jnp.where(keep.reshape(blocks, 1, 1), shaped, jnp.zeros((), BF)).reshape(rows, b)

        up = masked(l_up, m_up)
        lo = masked(l_lo, m_lo)
        a_across = send(a, CORE)
        scal = jnp.stack([h, (-x - z) % 4, col, v, x, g, place]).astype(jnp.int32)

        def spread(k0):
            o0 = send(k0, Y_HI)
            k3 = send(k0, Z_UP)
            k1 = send(k0, Z_DOWN)
            o3 = send(o0, Z_UP)
            o1 = send(o0, Z_DOWN)
            k2 = send(k3, Z_UP)
            o2 = send(o1, Z_DOWN)
            return k0, k1, k2, k3, o0, o1, o2, o3

        def reduce(parts):
            far_up, far_down, near_up, near_down, last_up, last_down, keep = parts
            far_up = send(far_up, X_UP)
            far_down = send(far_down, X_DOWN)
            near_up = send(near_up, X_UP)
            near_down = send(near_down, X_DOWN)
            last_up = (last_up.astype(F32) + far_up.astype(F32)).astype(BF)
            last_down = (last_down.astype(F32) + far_down.astype(F32)).astype(BF)
            last_up = send(last_up, X_UP)
            last_down = send(last_down, X_DOWN)
            mine = keep[:rows].astype(F32) + near_down.astype(F32) + last_up.astype(F32)
            other = keep[rows:].astype(F32) + near_up.astype(F32) + last_down.astype(F32)
            same = g == v
            first = jnp.where(same, other, mine).astype(BF)
            second = jnp.where(same, mine, other).astype(BF)
            first = send(first, LAST_A)
            second = send(second, LAST_B)
            return (-(first.astype(F32) + second.astype(F32))).astype(BF)

        up_pieces = spread(send(l_up, TURN))
        lo_first = send(after(lo, up_pieces[2]), TURN)

        lp_across = send(lp, Y_LO)
        own_col = jnp.concatenate([lo, lp, lp_across], 0)
        own_col = after(own_col, up_pieces[0])
        far = send(lo, Y_LO)
        n1, f1 = send(own_col, X_DOWN), send(far, X_DOWN)
        n2, f2 = send(own_col, X_FAR), send(far, X_FAR)
        n3, f3 = send(own_col, X_UP), send(far, X_UP)
        near_cols = (own_col, n1, n2, n3)
        cols = near_cols + (far, f1, f2, f3)

        parts = products(scal, a, a_across, up_pieces, (m_up,))
        lo_pieces = spread(after(lo_first, parts[0]))
        x_own = reduce(parts)
        lo_parts = products(scal, a, a_across, lo_pieces)
        x_across = send(x_own, CORE)

        parts = couple(scal, parent, lo_parts, x_own, x_across, near_cols)
        y_own = reduce(parts)

        upper, upper_given, kept, given = crossed(scal, parent, x_own, up, d_up, cols)
        terms = kept.astype(F32) + send(given, CORE).astype(F32)
        upper = upper + send(upper_given, CORE).astype(F32)
        half = b // 2
        diag = upper.astype(BF)
        diag = lax.all_to_all(jnp.broadcast_to(diag[None], (8, half, b)), "row", 0, 0, tiled=True)
        d_half = lax.dynamic_slice(d_up, (g * half, 0), (half, b)) - jnp.sum(diag.astype(F32), 0)
        terms = after(terms.astype(BF).reshape(64, piece, b), diag)
        terms = lax.all_to_all(terms, ("row", "col"), 0, 0, tiled=True)
        p_slice = (-jnp.sum(terms.astype(F32), 0)).astype(BF)

        own = dot(lo, y_own, (0, 0)) + dot(lp_slice, p_slice, (0, 0))
        own_given = lax.dynamic_slice(own, ((1 - g) * half, 0), (half, b)).astype(BF)
        own = lax.dynamic_slice(own, (g * half, 0), (half, b))
        own = (own + send(own_given, CORE).astype(F32)).astype(BF)
        own = jnp.concatenate([own, p_slice], 0)
        own = lax.all_to_all(jnp.broadcast_to(own[None], (8,) + own.shape), "row", 0, 0, tiled=True)
        last = lax.dynamic_slice(d_lo, (g * half, 0), (half, b)) - jnp.sum(
            own[:, :half].astype(F32), 0
        )
        y_parent = own[:, half:].reshape(half, b)
        mine = jnp.concatenate([d_half.astype(BF), y_parent, last.astype(BF)], 1)
        other = send(mine, CORE)

        def whole(part):
            ours, theirs = mine[:, part * b : (part + 1) * b], other[:, part * b : (part + 1) * b]
            return jnp.where(
                g == 0, jnp.concatenate([ours, theirs], 0), jnp.concatenate([theirs, ours], 0)
            )

        return x_own, whole(0), y_own, whole(1), whole(2)

    tall, flat, full = P(GR, "col"), P(None, "col"), P(None, None)
    return jax.shard_map(
        body,
        mesh=mesh,
        in_specs=(tall, tall, full, flat, tall, full, P(None), flat, flat),
        out_specs=(tall, flat, tall, flat, flat),
        check_vma=False,
    )
```

```python
import functools

import jax
import jax.numpy as jnp
import numpy as np
from jax import lax
from jax.experimental import pallas as pl
from jax.experimental.pallas import tpu as pltpu
from jax.sharding import PartitionSpec as P


ALL = ("grp", "row", "col")
GR = ("grp", "row")
SHAPE = (2, 4, 2, 2, 4)
BF = jnp.bfloat16
F32 = jnp.float32


def perm(move):
    pairs = []
    for place in np.ndindex(*SHAPE):
        target = move(*place)
        pairs.append(
            (int(np.ravel_multi_index(place, SHAPE)), int(np.ravel_multi_index(target, SHAPE)))
        )
    return pairs


TURN = perm(lambda g, z, h, v, x: (v, -x % 4, h, g, z))
CORE = perm(lambda g, z, h, v, x: (1 - g, z, h, v, x))
Y_HI = perm(lambda g, z, h, v, x: (g, z, 1 - h, v, x))
Y_LO = perm(lambda g, z, h, v, x: (g, z, h, 1 - v, x))
Z_FAR = perm(lambda g, z, h, v, x: (g, (z + 2) % 4, h, v, x))
Z_UP = perm(lambda g, z, h, v, x: (g, (z + 1) % 4, h, v, x))
Z_DOWN = perm(lambda g, z, h, v, x: (g, (z - 1) % 4, h, v, x))
X_FAR = perm(lambda g, z, h, v, x: (g, z, h, v, (x + 2) % 4))
X_UP = perm(lambda g, z, h, v, x: (g, z, h, v, (x + 1) % 4))
X_DOWN = perm(lambda g, z, h, v, x: (g, z, h, v, (x - 1) % 4))
LAST_A = perm(lambda g, z, h, v, x: (1 - g, z, h, v, x) if g == v else (g, z, h, 1 - v, x))
LAST_B = perm(lambda g, z, h, v, x: (g, z, h, v, x) if g == v else (1 - g, z, h, 1 - v, x))


def send(value, pairs):
    return lax.ppermute(value, ALL, pairs)


def dot(a, b, contract):
    return lax.dot_general(a, b, ((contract[:1], contract[1:]), ((), ())), preferred_element_type=F32)


def targets_of(rows):
    own, across = pl.ds(0, rows), pl.ds(rows, rows)
    return (
        (2, 0, 0, own),
        (3, 0, 3, own),
        (1, 0, 4, own),
        (0, 0, 6, own),
        (2, 1, 1, own),
        (1, 1, 2, own),
        (3, 1, 5, own),
        (0, 1, 6, across),
    )


def shapes_of(rows, b):
    short = jax.ShapeDtypeStruct((rows, b), BF)
    return [short] * 6 + [jax.ShapeDtypeStruct((2 * rows, b), BF)]


CHUNKS = 3


def products_kernel(depth, rows, scal, *refs):
    pieces = refs[2:10]
    mask, outs = refs[10:-13], refs[-13:-6]
    a_s, b_s, c_s, a_sems, b_sems, c_sems = refs[-6:]
    half, offset = scal[0], scal[1]
    size = rows // CHUNKS
    b = c_s.shape[2]

    def a_copy(chunk, part):
        which = half if part == 0 else 1 - half
        block, step = divmod(chunk, CHUNKS)
        return pltpu.make_async_copy(
            refs[block].at[
                pl.ds(step * size, size), pl.ds(pl.multiple_of(which * depth, depth), depth)
            ],
            a_s.at[pl.ds(chunk * size, size), pl.ds(part * depth, depth)],
            a_sems.at[chunk, part],
        )

    def b_copy(piece, slot, part):
        return pltpu.make_async_copy(
            pieces[piece],
            b_s.at[pl.ds(part * depth, depth), pl.ds(pl.multiple_of(slot * b, b), b)],
            b_sems.at[slot, part],
        )

    for part in range(2):
        a_copy(0, part).start()
        for k in range(4):
            b_copy(part * 4 + k, lax.rem(offset - k + 4, 4), part).start()
    for j in range(4):
        b_copy(0, j, 0).wait()
        b_copy(0, j, 1).wait()
    for chunk in range(1, 3):
        a_copy(chunk, 0).start()
        a_copy(chunk, 1).start()
    for j in range(4 if mask else 0):
        u = 4 * scal[5] + lax.rem(scal[4] + j, 4)
        for part in range(2):
            which = half if part == 0 else 1 - half
            for n in range(depth // b):

                @pl.when(mask[0][u, (2 * scal[2] + which) * (depth // b) + n] <= 0)
                def _():
                    b_s[pl.ds(part * depth + n * b, b), pl.ds(j * b, b)] = jnp.zeros((b, b), BF)

    copies = []
    for chunk in range(2 * CHUNKS):
        a_copy(chunk, 0).wait()
        a_copy(chunk, 1).wait()
        if chunk + 3 < 2 * CHUNKS:
            a_copy(chunk + 3, 0).start()
            a_copy(chunk + 3, 1).start()
        block, step = divmod(chunk, CHUNKS)
        total = jnp.dot(
            a_s[pl.ds(chunk * size, size), :], b_s[...], preferred_element_type=F32
        ).astype(BF)
        for n, (j, where, out, place) in enumerate(targets_of(rows)):
            if where == block:
                c_s[n, pl.ds(step * size, size), :] = total[:, j * b : (j + 1) * b]
                copies.append(
                    pltpu.make_async_copy(
                        c_s.at[n, pl.ds(step * size, size), :],
                        outs[out].at[pl.ds(place.start + step * size, size), :],
                        c_sems.at[n, step],
                    )
                )
                copies[-1].start()
    for copy in copies:
        copy.wait()


def products(scal, a, a_across, pieces, mask=()):
    rows, width = a.shape
    depth, b = pieces[0].shape
    hbm = pl.BlockSpec(memory_space=pl.ANY)
    smem = pl.BlockSpec(memory_space=pltpu.SMEM)
    return pl.pallas_call(
        functools.partial(products_kernel, depth, rows),
        out_shape=shapes_of(rows, b),
        in_specs=[smem] + [hbm] * 10 + [smem] * len(mask),
        out_specs=[hbm] * 7,
        scratch_shapes=[
            pltpu.VMEM((2 * rows, width), BF),
            pltpu.VMEM((width, 4 * b), BF),
            pltpu.VMEM((8, rows, b), BF),
            pltpu.SemaphoreType.DMA((2 * CHUNKS, 2)),
            pltpu.SemaphoreType.DMA((4, 2)),
            pltpu.SemaphoreType.DMA((8, CHUNKS)),
        ],
        cost_estimate=pl.CostEstimate(
            flops=2 * 2 * rows * width * 4 * b, bytes_accessed=12_000_000, transcendentals=0
        ),
        compiler_params=pltpu.CompilerParams(vmem_limit_bytes=60 * 1024 * 1024),
        name="products",
    )(scal, a, a_across, *pieces, *mask)


def panel_at(n, rows):
    return n, 0, 0, rows


def link_at(n, rows, b):
    return n % 4, rows + n // 4 * b, rows, b


def couple_kernel(rows, scal, parent, x_own, x_across, *refs):
    cols, outs = refs[:4], refs[11:18]
    blocks, links, in_sems, out_sems, link_sems = refs[18:]
    col, v, x, g = scal[2], scal[3], scal[4], scal[5]
    b = links.shape[1]

    def used(j):
        return parent[4 * g + lax.rem(x + j, 4)] == col

    def block_in(n, out, place):
        return pltpu.make_async_copy(outs[out].at[place, :], blocks.at[n], in_sems.at[n])

    def block_out(n, out, place):
        return pltpu.make_async_copy(blocks.at[n], outs[out].at[place, :], out_sems.at[n])

    def link_in(j, far):
        buffer, start, _, size = link_at(j + 4 * far, rows, b)
        return pltpu.make_async_copy(
            cols[buffer].at[pl.ds(start, size), :], links.at[j], link_sems.at[j]
        )

    for j in range(4):
        for far in range(2):

            @pl.when(jnp.logical_and(used(j), (g == v) == (far == 0)))
            def _():
                link_in(j, far).start()

    for n, (j, block, out, place) in enumerate(targets_of(rows)):

        @pl.when(used(j))
        def _():
            block_in(n, out, place).start()

    for n, (j, block, out, place) in enumerate(targets_of(rows)):

        @pl.when(used(j))
        def _():
            if block == 0:
                link_in(j, 0).wait()
            block_in(n, out, place).wait()
            value = (x_own, x_across)[block]
            total = jnp.dot(value[...], links[j], preferred_element_type=F32)
            blocks[n] = (blocks[n].astype(F32) + total).astype(BF)
            block_out(n, out, place).start()

    for n, (j, block, out, place) in enumerate(targets_of(rows)):

        @pl.when(used(j))
        def _():
            block_out(n, out, place).wait()


def couple(scal, parent, parts, x_own, x_across, cols):
    rows, b = x_own.shape
    smem = pl.BlockSpec(memory_space=pltpu.SMEM)
    vmem = pl.BlockSpec(memory_space=pltpu.VMEM)
    hbm = pl.BlockSpec(memory_space=pl.ANY)
    return pl.pallas_call(
        functools.partial(couple_kernel, rows),
        out_shape=[jax.ShapeDtypeStruct(p.shape, BF) for p in parts],
        in_specs=[smem, smem, vmem, vmem] + [hbm] * 11,
        out_specs=[hbm] * 7,
        scratch_shapes=[
            pltpu.VMEM((8, rows, b), BF),
            pltpu.VMEM((4, b, b), BF),
            pltpu.SemaphoreType.DMA((8,)),
            pltpu.SemaphoreType.DMA((8,)),
            pltpu.SemaphoreType.DMA((4,)),
        ],
        input_output_aliases={8 + n: n for n in range(7)},
        cost_estimate=pl.CostEstimate(
            flops=2 * 2 * rows * b * 4 * b, bytes_accessed=8_000_000, transcendentals=0
        ),
        compiler_params=pltpu.CompilerParams(vmem_limit_bytes=60 * 1024 * 1024),
        name="couple",
    )(scal, parent, x_own, x_across, *cols, *parts)


def crossed_kernel(rows, scal, parent, x_ref, up_ref, d_ref, *refs):
    cols, outs, (held, whole, sems) = refs[:8], refs[8:12], refs[12:]
    upper_kept, upper_given, kept, given = outs
    col, v, x, g, place = scal[2], scal[3], scal[4], scal[5], scal[6]
    slices, _, piece, b = kept.shape
    half = b // 2
    ours = pl.ds(pl.multiple_of(g * half, half), half)
    theirs = pl.ds(pl.multiple_of((1 - g) * half, half), half)

    def child(n):
        side = v if n < 4 else 1 - v
        return 4 * side + lax.rem(x + n % 4, 4)

    def fetch(n):
        parts = (panel_at(n, rows), link_at(n, rows, b))
        return [
            pltpu.make_async_copy(
                cols[source].at[pl.ds(start, size), :],
                held.at[n, pl.ds(to, size), :],
                sems.at[n, m],
            )
            for m, (source, start, to, size) in enumerate(parts)
        ]

    for n in range(8):

        @pl.when(parent[child(n)] == col)
        def _():
            for copy in fetch(n):
                copy.start()

    total = dot(up_ref[...], x_ref[...], (0, 0))
    whole[...] = total
    upper_kept[...] = whole[ours, :]
    upper_given[...] = whole[theirs, :].astype(BF)
    first = jnp.where(place == 0, 1.0, 0.0)
    diag = (d_ref[...] * first - total).astype(BF)
    for n in range(8):
        l = child(n)

        @pl.when(parent[l] == col)
        def _():
            for copy in fetch(n):
                copy.wait()
            term = dot(x_ref[...], held[n, pl.ds(0, rows), :], (0, 0))
            term += dot(diag, held[n, pl.ds(rows, b), :], (1, 0))
            whole[...] = term
            kept[:, l] = whole[ours, :].astype(BF).reshape(slices, piece, b)
            given[:, l] = whole[theirs, :].astype(BF).reshape(slices, piece, b)

        @pl.when(parent[l] != col)
        def _():
            kept[:, l] = jnp.zeros((slices, piece, b), BF)
            given[:, l] = jnp.zeros((slices, piece, b), BF)


def crossed(scal, parent, x, up, d_up, cols):
    rows, b = x.shape
    smem = pl.BlockSpec(memory_space=pltpu.SMEM)
    vmem = pl.BlockSpec(memory_space=pltpu.VMEM)
    hbm = pl.BlockSpec(memory_space=pl.ANY)
    return pl.pallas_call(
        functools.partial(crossed_kernel, rows),
        out_shape=[
            jax.ShapeDtypeStruct((b // 2, b), F32),
            jax.ShapeDtypeStruct((b // 2, b), BF),
            jax.ShapeDtypeStruct((8, 8, b // 16, b), BF),
            jax.ShapeDtypeStruct((8, 8, b // 16, b), BF),
        ],
        in_specs=[smem, smem, vmem, vmem, vmem] + [hbm] * 8,
        out_specs=[vmem] * 4,
        scratch_shapes=[
            pltpu.VMEM((8, rows + b, b), BF),
            pltpu.VMEM((b, b), F32),
            pltpu.SemaphoreType.DMA((8, 2)),
        ],
        cost_estimate=pl.CostEstimate(
            flops=2 * rows * b * 8 * b, bytes_accessed=5_000_000, transcendentals=0
        ),
        compiler_params=pltpu.CompilerParams(vmem_limit_bytes=60 * 1024 * 1024),
        name="crossed",
    )(scal, parent, x, up, d_up, *cols)


def after(value, *others):
    return lax.optimization_barrier((value,) + others)[0]


def solution(mesh):
    def body(a, l_up, m_up, d_up, l_lo, m_lo, parent, lp, d_lo):
        rows, b = l_up.shape
        blocks = rows // b
        piece = b // 16
        g, row, col = lax.axis_index("grp"), lax.axis_index("row"), lax.axis_index("col")
        z, h = row // 2, row % 2
        v, x = col // 4, col % 4
        place = g * 8 + row

        lp_slice = lax.optimization_barrier(lax.dynamic_slice(lp, (place * piece, 0), (piece, b)))

        def masked(factor, pattern):
            keep = lax.dynamic_slice(pattern, (col, place * blocks), (1, blocks)) > 0
            shaped = factor.reshape(blocks, b, b)
            return jnp.where(keep.reshape(blocks, 1, 1), shaped, jnp.zeros((), BF)).reshape(rows, b)

        up, lo = masked(l_up, m_up), masked(l_lo, m_lo)
        a_across = send(a, CORE)
        scal = jnp.stack([h, (-x - z) % 4, col, v, x, g, place]).astype(jnp.int32)

        def spread(k0):
            o0 = send(k0, Y_HI)
            k3 = send(k0, Z_UP)
            k1 = send(k0, Z_DOWN)
            o3 = send(o0, Z_UP)
            o1 = send(o0, Z_DOWN)
            k2 = send(k3, Z_UP)
            o2 = send(o1, Z_DOWN)
            return k0, k1, k2, k3, o0, o1, o2, o3

        def reduce(parts):
            far_up, far_down, near_up, near_down, last_up, last_down, keep = parts
            far_up = send(far_up, X_UP)
            far_down = send(far_down, X_DOWN)
            near_up = send(near_up, X_UP)
            near_down = send(near_down, X_DOWN)
            last_up = (last_up.astype(F32) + far_up.astype(F32)).astype(BF)
            last_down = (last_down.astype(F32) + far_down.astype(F32)).astype(BF)
            last_up = send(last_up, X_UP)
            last_down = send(last_down, X_DOWN)
            mine = keep[:rows].astype(F32) + near_down.astype(F32) + last_up.astype(F32)
            other = keep[rows:].astype(F32) + near_up.astype(F32) + last_down.astype(F32)
            same = g == v
            first = jnp.where(same, other, mine).astype(BF)
            second = jnp.where(same, mine, other).astype(BF)
            first = send(first, LAST_A)
            second = send(second, LAST_B)
            return (-(first.astype(F32) + second.astype(F32))).astype(BF)

        up_pieces = spread(send(l_up, TURN))
        lo_first = send(after(lo, up_pieces[2]), TURN)

        lp_across = send(lp, Y_LO)
        own_col = jnp.concatenate([lo, lp, lp_across], 0)
        own_col = after(own_col, up_pieces[0])
        far = send(lo, Y_LO)
        n1, f1 = send(own_col, X_DOWN), send(far, X_DOWN)
        n2, f2 = send(own_col, X_FAR), send(far, X_FAR)
        n3, f3 = send(own_col, X_UP), send(far, X_UP)
        near_cols = (own_col, n1, n2, n3)
        cols = near_cols + (far, f1, f2, f3)

        parts = products(scal, a, a_across, up_pieces, (m_up,))
        lo_pieces = spread(after(lo_first, parts[0]))
        x_own = reduce(parts)
        lo_parts = products(scal, a, a_across, lo_pieces)
        x_across = send(x_own, CORE)

        parts = couple(scal, parent, lo_parts, x_own, x_across, near_cols)
        y_own = reduce(parts)

        upper, upper_given, kept, given = crossed(scal, parent, x_own, up, d_up, cols)
        terms = kept.astype(F32) + send(given, CORE).astype(F32)
        upper = upper + send(upper_given, CORE).astype(F32)
        terms = terms.astype(BF).reshape(64, piece, b)
        terms = lax.all_to_all(terms, ("row", "col"), 0, 0, tiled=True)
        p_slice = (-jnp.sum(terms.astype(F32), 0)).astype(BF)

        half = b // 2
        upper = upper.astype(BF)
        pair = (upper.astype(F32) + send(upper, Y_HI).astype(F32)).astype(BF)
        line = [send(pair, way) for way in (Z_FAR, Z_UP, Z_DOWN)]
        far_sum = pair.astype(F32) + line[0].astype(F32)
        near_sum = line[1].astype(F32) + line[2].astype(F32)
        d_half = lax.dynamic_slice(d_up, (g * half, 0), (half, b)) - (far_sum + near_sum)

        own = dot(lo, y_own, (0, 0)) + dot(lp_slice, p_slice, (0, 0))
        own_given = lax.dynamic_slice(own, ((1 - g) * half, 0), (half, b)).astype(BF)
        own = lax.dynamic_slice(own, (g * half, 0), (half, b))
        own = (own + send(own_given, CORE).astype(F32)).astype(BF)
        own = jnp.concatenate([own, p_slice], 0)
        own = lax.all_to_all(jnp.broadcast_to(own[None], (8,) + own.shape), "row", 0, 0, tiled=True)
        last = lax.dynamic_slice(d_lo, (g * half, 0), (half, b)) - jnp.sum(
            own[:, :half].astype(F32), 0
        )
        y_parent = own[:, half:].reshape(half, b)
        mine = jnp.concatenate([d_half.astype(BF), y_parent, last.astype(BF)], 1)
        other = send(mine, CORE)

        def whole(part):
            ours, theirs = mine[:, part * b : (part + 1) * b], other[:, part * b : (part + 1) * b]
            return jnp.where(
                g == 0, jnp.concatenate([ours, theirs], 0), jnp.concatenate([theirs, ours], 0)
            )

        return x_own, whole(0), y_own, whole(1), whole(2)

    tall, flat, full = P(GR, "col"), P(None, "col"), P(None, None)
    return jax.shard_map(
        body,
        mesh=mesh,
        in_specs=(tall, tall, full, flat, tall, full, P(None), flat, flat),
        out_specs=(tall, flat, tall, flat, flat),
        check_vma=False,
    )
```

```python
import functools

import jax
import jax.numpy as jnp
import numpy as np
from jax import lax
from jax.experimental import pallas as pl
from jax.experimental.pallas import tpu as pltpu
from jax.sharding import PartitionSpec as P


ALL = ("grp", "row", "col")
GR = ("grp", "row")
SHAPE = (2, 4, 2, 2, 4)
BF = jnp.bfloat16
F32 = jnp.float32


def perm(move):
    pairs = []
    for place in np.ndindex(*SHAPE):
        target = move(*place)
        pairs.append(
            (int(np.ravel_multi_index(place, SHAPE)), int(np.ravel_multi_index(target, SHAPE)))
        )
    return pairs


TURN = perm(lambda g, z, h, v, x: (v, -x % 4, h, g, z))
CORE = perm(lambda g, z, h, v, x: (1 - g, z, h, v, x))
Y_HI = perm(lambda g, z, h, v, x: (g, z, 1 - h, v, x))
Y_LO = perm(lambda g, z, h, v, x: (g, z, h, 1 - v, x))
Z_FAR = perm(lambda g, z, h, v, x: (g, (z + 2) % 4, h, v, x))
Z_UP = perm(lambda g, z, h, v, x: (g, (z + 1) % 4, h, v, x))
Z_DOWN = perm(lambda g, z, h, v, x: (g, (z - 1) % 4, h, v, x))
X_FAR = perm(lambda g, z, h, v, x: (g, z, h, v, (x + 2) % 4))
X_UP = perm(lambda g, z, h, v, x: (g, z, h, v, (x + 1) % 4))
X_DOWN = perm(lambda g, z, h, v, x: (g, z, h, v, (x - 1) % 4))
LAST_A = perm(lambda g, z, h, v, x: (1 - g, z, h, v, x) if g == v else (g, z, h, 1 - v, x))
LAST_B = perm(lambda g, z, h, v, x: (g, z, h, v, x) if g == v else (1 - g, z, h, 1 - v, x))


def send(value, pairs):
    return lax.ppermute(value, ALL, pairs)


def dot(a, b, contract):
    return lax.dot_general(a, b, ((contract[:1], contract[1:]), ((), ())), preferred_element_type=F32)


def targets_of(rows):
    own, across = pl.ds(0, rows), pl.ds(rows, rows)
    return (
        (2, 0, 0, own),
        (3, 0, 3, own),
        (1, 0, 4, own),
        (0, 0, 6, own),
        (2, 1, 1, own),
        (1, 1, 2, own),
        (3, 1, 5, own),
        (0, 1, 6, across),
    )


def shapes_of(rows, b):
    short = jax.ShapeDtypeStruct((rows, b), BF)
    return [short] * 6 + [jax.ShapeDtypeStruct((2 * rows, b), BF)]


CHUNKS = 3


def products_kernel(depth, rows, scal, *refs):
    pieces = refs[2:10]
    mask, outs = refs[10:-13], refs[-13:-6]
    a_s, b_s, c_s, a_sems, b_sems, c_sems = refs[-6:]
    half, offset = scal[0], scal[1]
    size = rows // CHUNKS
    b = c_s.shape[2]

    def a_copy(chunk, part):
        which = half if part == 0 else 1 - half
        block, step = divmod(chunk, CHUNKS)
        return pltpu.make_async_copy(
            refs[block].at[
                pl.ds(step * size, size), pl.ds(pl.multiple_of(which * depth, depth), depth)
            ],
            a_s.at[pl.ds(chunk * size, size), pl.ds(part * depth, depth)],
            a_sems.at[chunk, part],
        )

    def b_copy(piece, slot, part):
        return pltpu.make_async_copy(
            pieces[piece],
            b_s.at[pl.ds(part * depth, depth), pl.ds(pl.multiple_of(slot * b, b), b)],
            b_sems.at[slot, part],
        )

    for part in range(2):
        a_copy(0, part).start()
        for k in range(4):
            b_copy(part * 4 + k, lax.rem(offset - k + 4, 4), part).start()

    def arrive(part):
        a_copy(0, part).wait()
        for j in range(4):
            b_copy(0, j, part).wait()
            for n in range(depth // b if mask else 0):
                u = 4 * scal[5] + lax.rem(scal[4] + j, 4)
                which = half if part == 0 else 1 - half

                @pl.when(mask[0][u, (2 * scal[2] + which) * (depth // b) + n] <= 0)
                def _():
                    b_s[pl.ds(part * depth + n * b, b), pl.ds(j * b, b)] = jnp.zeros((b, b), BF)

    def product(chunk, span):
        return jnp.dot(
            a_s[pl.ds(chunk * size, size), span], b_s[span, :], preferred_element_type=F32
        )

    copies = []
    for chunk in range(2 * CHUNKS):
        if chunk == 0:
            arrive(0)
            total = product(chunk, pl.ds(0, depth))
            arrive(1)
            for later in range(1, 3):
                a_copy(later, 0).start()
                a_copy(later, 1).start()
            total = (total + product(chunk, pl.ds(depth, depth))).astype(BF)
        else:
            a_copy(chunk, 0).wait()
            a_copy(chunk, 1).wait()
            total = product(chunk, pl.ds(0, 2 * depth)).astype(BF)
        if chunk + 3 < 2 * CHUNKS:
            a_copy(chunk + 3, 0).start()
            a_copy(chunk + 3, 1).start()
        block, step = divmod(chunk, CHUNKS)
        for n, (j, where, out, place) in enumerate(targets_of(rows)):
            if where == block:
                c_s[n, pl.ds(step * size, size), :] = total[:, j * b : (j + 1) * b]
                copies.append(
                    pltpu.make_async_copy(
                        c_s.at[n, pl.ds(step * size, size), :],
                        outs[out].at[pl.ds(place.start + step * size, size), :],
                        c_sems.at[n, step],
                    )
                )
                copies[-1].start()
    for copy in copies:
        copy.wait()


def products(scal, a, a_across, pieces, mask=()):
    rows, width = a.shape
    depth, b = pieces[0].shape
    hbm = pl.BlockSpec(memory_space=pl.ANY)
    smem = pl.BlockSpec(memory_space=pltpu.SMEM)
    return pl.pallas_call(
        functools.partial(products_kernel, depth, rows),
        out_shape=shapes_of(rows, b),
        in_specs=[smem] + [hbm] * 10 + [smem] * len(mask),
        out_specs=[hbm] * 7,
        scratch_shapes=[
            pltpu.VMEM((2 * rows, width), BF),
            pltpu.VMEM((width, 4 * b), BF),
            pltpu.VMEM((8, rows, b), BF),
            pltpu.SemaphoreType.DMA((2 * CHUNKS, 2)),
            pltpu.SemaphoreType.DMA((4, 2)),
            pltpu.SemaphoreType.DMA((8, CHUNKS)),
        ],
        cost_estimate=pl.CostEstimate(
            flops=2 * 2 * rows * width * 4 * b, bytes_accessed=12_000_000, transcendentals=0
        ),
        compiler_params=pltpu.CompilerParams(vmem_limit_bytes=60 * 1024 * 1024),
        name="products",
    )(scal, a, a_across, *pieces, *mask)


def panel_at(n, rows):
    return n, 0, 0, rows


def link_at(n, rows, b):
    return n % 4, rows + n // 4 * b, rows, b


def couple_kernel(rows, scal, parent, x_own, x_across, *refs):
    cols, outs = refs[:4], refs[11:18]
    blocks, links, in_sems, out_sems, link_sems = refs[18:]
    col, v, x, g = scal[2], scal[3], scal[4], scal[5]
    b = links.shape[1]

    def used(j):
        return parent[4 * g + lax.rem(x + j, 4)] == col

    def block_in(n, out, place):
        return pltpu.make_async_copy(outs[out].at[place, :], blocks.at[n], in_sems.at[n])

    def block_out(n, out, place):
        return pltpu.make_async_copy(blocks.at[n], outs[out].at[place, :], out_sems.at[n])

    def link_in(j, far):
        buffer, start, _, size = link_at(j + 4 * far, rows, b)
        return pltpu.make_async_copy(
            cols[buffer].at[pl.ds(start, size), :], links.at[j], link_sems.at[j]
        )

    for j in range(4):
        for far in range(2):

            @pl.when(jnp.logical_and(used(j), (g == v) == (far == 0)))
            def _():
                link_in(j, far).start()

    for n, (j, block, out, place) in enumerate(targets_of(rows)):

        @pl.when(used(j))
        def _():
            block_in(n, out, place).start()

    for n, (j, block, out, place) in enumerate(targets_of(rows)):

        @pl.when(used(j))
        def _():
            if block == 0:
                link_in(j, 0).wait()
            block_in(n, out, place).wait()
            value = (x_own, x_across)[block]
            total = jnp.dot(value[...], links[j], preferred_element_type=F32)
            blocks[n] = (blocks[n].astype(F32) + total).astype(BF)
            block_out(n, out, place).start()

    for n, (j, block, out, place) in enumerate(targets_of(rows)):

        @pl.when(used(j))
        def _():
            block_out(n, out, place).wait()


def couple(scal, parent, parts, x_own, x_across, cols):
    rows, b = x_own.shape
    smem = pl.BlockSpec(memory_space=pltpu.SMEM)
    vmem = pl.BlockSpec(memory_space=pltpu.VMEM)
    hbm = pl.BlockSpec(memory_space=pl.ANY)
    return pl.pallas_call(
        functools.partial(couple_kernel, rows),
        out_shape=[jax.ShapeDtypeStruct(p.shape, BF) for p in parts],
        in_specs=[smem, smem, vmem, vmem] + [hbm] * 11,
        out_specs=[hbm] * 7,
        scratch_shapes=[
            pltpu.VMEM((8, rows, b), BF),
            pltpu.VMEM((4, b, b), BF),
            pltpu.SemaphoreType.DMA((8,)),
            pltpu.SemaphoreType.DMA((8,)),
            pltpu.SemaphoreType.DMA((4,)),
        ],
        input_output_aliases={8 + n: n for n in range(7)},
        cost_estimate=pl.CostEstimate(
            flops=2 * 2 * rows * b * 4 * b, bytes_accessed=8_000_000, transcendentals=0
        ),
        compiler_params=pltpu.CompilerParams(vmem_limit_bytes=60 * 1024 * 1024),
        name="couple",
    )(scal, parent, x_own, x_across, *cols, *parts)


def crossed_kernel(rows, scal, parent, x_ref, up_ref, d_ref, *refs):
    cols, outs, (held, whole, sems) = refs[:8], refs[8:12], refs[12:]
    upper_kept, upper_given, kept, given = outs
    col, v, x, g, place = scal[2], scal[3], scal[4], scal[5], scal[6]
    slices, _, piece, b = kept.shape
    half = b // 2
    ours = pl.ds(pl.multiple_of(g * half, half), half)
    theirs = pl.ds(pl.multiple_of((1 - g) * half, half), half)

    def child(n):
        side = v if n < 4 else 1 - v
        return 4 * side + lax.rem(x + n % 4, 4)

    def fetch(n):
        parts = (panel_at(n, rows), link_at(n, rows, b))
        return [
            pltpu.make_async_copy(
                cols[source].at[pl.ds(start, size), :],
                held.at[n, pl.ds(to, size), :],
                sems.at[n, m],
            )
            for m, (source, start, to, size) in enumerate(parts)
        ]

    for n in range(8):

        @pl.when(parent[child(n)] == col)
        def _():
            for copy in fetch(n):
                copy.start()

    total = dot(up_ref[...], x_ref[...], (0, 0))
    whole[...] = total
    upper_kept[...] = whole[ours, :]
    upper_given[...] = whole[theirs, :].astype(BF)
    first = jnp.where(place == 0, 1.0, 0.0)
    diag = (d_ref[...] * first - total).astype(BF)
    for n in range(8):
        l = child(n)

        @pl.when(parent[l] == col)
        def _():
            for copy in fetch(n):
                copy.wait()
            term = dot(x_ref[...], held[n, pl.ds(0, rows), :], (0, 0))
            term += dot(diag, held[n, pl.ds(rows, b), :], (1, 0))
            whole[...] = term
            kept[:, l] = whole[ours, :].astype(BF).reshape(slices, piece, b)
            given[:, l] = whole[theirs, :].astype(BF).reshape(slices, piece, b)

        @pl.when(parent[l] != col)
        def _():
            kept[:, l] = jnp.zeros((slices, piece, b), BF)
            given[:, l] = jnp.zeros((slices, piece, b), BF)


def crossed(scal, parent, x, up, d_up, cols):
    rows, b = x.shape
    smem = pl.BlockSpec(memory_space=pltpu.SMEM)
    vmem = pl.BlockSpec(memory_space=pltpu.VMEM)
    hbm = pl.BlockSpec(memory_space=pl.ANY)
    return pl.pallas_call(
        functools.partial(crossed_kernel, rows),
        out_shape=[
            jax.ShapeDtypeStruct((b // 2, b), F32),
            jax.ShapeDtypeStruct((b // 2, b), BF),
            jax.ShapeDtypeStruct((8, 8, b // 16, b), BF),
            jax.ShapeDtypeStruct((8, 8, b // 16, b), BF),
        ],
        in_specs=[smem, smem, vmem, vmem, vmem] + [hbm] * 8,
        out_specs=[vmem] * 4,
        scratch_shapes=[
            pltpu.VMEM((8, rows + b, b), BF),
            pltpu.VMEM((b, b), F32),
            pltpu.SemaphoreType.DMA((8, 2)),
        ],
        cost_estimate=pl.CostEstimate(
            flops=2 * rows * b * 8 * b, bytes_accessed=5_000_000, transcendentals=0
        ),
        compiler_params=pltpu.CompilerParams(vmem_limit_bytes=60 * 1024 * 1024),
        name="crossed",
    )(scal, parent, x, up, d_up, *cols)


def after(value, *others):
    return lax.optimization_barrier((value,) + others)[0]


def solution(mesh):
    def body(a, l_up, m_up, d_up, l_lo, m_lo, parent, lp, d_lo):
        rows, b = l_up.shape
        blocks = rows // b
        piece = b // 16
        g, row, col = lax.axis_index("grp"), lax.axis_index("row"), lax.axis_index("col")
        z, h = row // 2, row % 2
        v, x = col // 4, col % 4
        place = g * 8 + row

        lp_slice = lax.optimization_barrier(lax.dynamic_slice(lp, (place * piece, 0), (piece, b)))

        def masked(factor, pattern):
            keep = lax.dynamic_slice(pattern, (col, place * blocks), (1, blocks)) > 0
            shaped = factor.reshape(blocks, b, b)
            return jnp.where(keep.reshape(blocks, 1, 1), shaped, jnp.zeros((), BF)).reshape(rows, b)

        up, lo = masked(l_up, m_up), masked(l_lo, m_lo)
        a_across = send(a, CORE)
        scal = jnp.stack([h, (-x - z) % 4, col, v, x, g, place]).astype(jnp.int32)

        def spread(k0):
            o0 = send(k0, Y_HI)
            k3 = send(k0, Z_UP)
            k1 = send(k0, Z_DOWN)
            o3 = send(o0, Z_UP)
            o1 = send(o0, Z_DOWN)
            k2 = send(k3, Z_UP)
            o2 = send(o1, Z_DOWN)
            return k0, k1, k2, k3, o0, o1, o2, o3

        def reduce(parts):
            far_up, far_down, near_up, near_down, last_up, last_down, keep = parts
            far_up = send(far_up, X_UP)
            far_down = send(far_down, X_DOWN)
            near_up = send(near_up, X_UP)
            near_down = send(near_down, X_DOWN)
            last_up = (last_up.astype(F32) + far_up.astype(F32)).astype(BF)
            last_down = (last_down.astype(F32) + far_down.astype(F32)).astype(BF)
            last_up = send(last_up, X_UP)
            last_down = send(last_down, X_DOWN)
            mine = keep[:rows].astype(F32) + near_down.astype(F32) + last_up.astype(F32)
            other = keep[rows:].astype(F32) + near_up.astype(F32) + last_down.astype(F32)
            same = g == v
            first = jnp.where(same, other, mine).astype(BF)
            second = jnp.where(same, mine, other).astype(BF)
            first = send(first, LAST_A)
            second = send(second, LAST_B)
            return (-(first.astype(F32) + second.astype(F32))).astype(BF)

        up_pieces = spread(send(l_up, TURN))
        lo_first = send(after(lo, up_pieces[2]), TURN)

        lp_across = send(lp, Y_LO)
        own_col = jnp.concatenate([lo, lp, lp_across], 0)
        own_col = after(own_col, up_pieces[0])
        far = send(lo, Y_LO)
        n1, f1 = send(own_col, X_DOWN), send(far, X_DOWN)
        n2, f2 = send(own_col, X_FAR), send(far, X_FAR)
        n3, f3 = send(own_col, X_UP), send(far, X_UP)
        near_cols = (own_col, n1, n2, n3)
        cols = near_cols + (far, f1, f2, f3)

        parts = products(scal, a, a_across, up_pieces, (m_up,))
        lo_pieces = spread(after(lo_first, parts[0]))
        x_own = reduce(parts)
        lo_parts = products(scal, a, a_across, lo_pieces)
        x_across = send(x_own, CORE)

        parts = couple(scal, parent, lo_parts, x_own, x_across, near_cols)
        y_own = reduce(parts)

        upper, upper_given, kept, given = crossed(scal, parent, x_own, up, d_up, cols)
        terms = kept.astype(F32) + send(given, CORE).astype(F32)
        upper = upper + send(upper_given, CORE).astype(F32)
        terms = terms.astype(BF).reshape(64, piece, b)
        terms = lax.all_to_all(terms, ("row", "col"), 0, 0, tiled=True)
        p_slice = (-jnp.sum(terms.astype(F32), 0)).astype(BF)

        half = b // 2
        upper = upper.astype(BF)
        pair = (upper.astype(F32) + send(upper, Y_HI).astype(F32)).astype(BF)
        line = [send(pair, way) for way in (Z_FAR, Z_UP, Z_DOWN)]
        far_sum = pair.astype(F32) + line[0].astype(F32)
        near_sum = line[1].astype(F32) + line[2].astype(F32)
        d_half = lax.dynamic_slice(d_up, (g * half, 0), (half, b)) - (far_sum + near_sum)

        own = dot(lo, y_own, (0, 0)) + dot(lp_slice, p_slice, (0, 0))
        own_given = lax.dynamic_slice(own, ((1 - g) * half, 0), (half, b)).astype(BF)
        own = lax.dynamic_slice(own, (g * half, 0), (half, b))
        own = (own + send(own_given, CORE).astype(F32)).astype(BF)
        own = jnp.concatenate([own, p_slice], 0)
        own = lax.all_to_all(jnp.broadcast_to(own[None], (8,) + own.shape), "row", 0, 0, tiled=True)
        last = lax.dynamic_slice(d_lo, (g * half, 0), (half, b)) - jnp.sum(
            own[:, :half].astype(F32), 0
        )
        y_parent = own[:, half:].reshape(half, b)
        mine = jnp.concatenate([d_half.astype(BF), y_parent, last.astype(BF)], 1)
        other = send(mine, CORE)

        def whole(part):
            ours, theirs = mine[:, part * b : (part + 1) * b], other[:, part * b : (part + 1) * b]
            return jnp.where(
                g == 0, jnp.concatenate([ours, theirs], 0), jnp.concatenate([theirs, ours], 0)
            )

        return x_own, whole(0), y_own, whole(1), whole(2)

    tall, flat, full = P(GR, "col"), P(None, "col"), P(None, None)
    return jax.shard_map(
        body,
        mesh=mesh,
        in_specs=(tall, tall, full, flat, tall, full, P(None), flat, flat),
        out_specs=(tall, flat, tall, flat, flat),
        check_vma=False,
    )
```
